32 devices in a mesh: grp: 2 (over core), ep: 16 (over z, y, x).
Axes of the slice: x: 2, y: 2, z: 4, core: 2. Of those that a mesh axis runs over, the one named last changes fastest.
Arguments:
- tokens: float32 [512, 6144], P('ep'), may hold values from -6 to 6
- route_ids: int32 [512, 12], P('ep'), may hold values from 0 to 95, as said below
- route_weights: float32 [512, 12], P('ep'), may hold values from 0.05 to 1
- expert_rows: float32 [64, 96, 6144], P(('grp', 'ep')), may hold values from -6 to 6
Outputs:
- combined: float32 [512, 6144], P('ep', 'grp')
The draws below stay inside these ranges and needn't reach their ends.
Inputs may be any that keep to these rules, and one draw needn't show every extreme that they name: `route_ids`: each row names 12 different experts. Each routed expert is chosen by at most 96 tokens in all, and by at most 6 of the 32 tokens of one ep index; some routed expert reaches each of these bounds in every draw. Values 64 and above are identity experts.
All inputs are finite; a program needn't handle non-finite values.
Results may differ from the reference program's by a relative error of at most 0.00002.
Values sent between devices are 32-bit elements; how exact they have to be, the bound alone decides.
A program may use at most 64 MiB of HBM per device.

```python
import math
import jax
import jax.numpy as jnp
import numpy as np

D = 6144
TOP = 12
TOK_DEV = 32
TOKENS = 512
EXPERTS = 64
ZEXP = 32
LANE = 8
CAP = 96
N_GRP = 2


def quota_table():
    rest = TOKENS - CAP - CAP // 2
    base = rest // (LANE - 2)
    extra = rest % (LANE - 2)
    table = [CAP, CAP // 2] + [base + (1 if j < extra else 0) for j in range(LANE - 2)]
    return np.array(table, dtype=np.int32)


def draw_route_ids(key, part):
    key = jax.random.fold_in(key, 7311)
    homes = TOKENS // TOK_DEV
    quotas = jnp.asarray(quota_table())
    values = jnp.repeat(jnp.arange(LANE, dtype=jnp.int32), quotas, total_repeat_length=TOKENS)
    key_real, key_rest, key_lanes = jax.random.split(key, 3)
    real_order = jax.random.permutation(key_real, EXPERTS).astype(jnp.int32)
    others = jnp.concatenate([real_order[TOP:], EXPERTS + jnp.arange(ZEXP, dtype=jnp.int32)])
    others = jax.random.permutation(key_rest, others).astype(jnp.int32)
    labels = jnp.concatenate([real_order[:TOP][:, None], others.reshape(TOP, LANE - 1)], axis=1)
    columns = []
    lane_keys = jax.random.split(key_lanes, TOP)
    for lane in range(TOP):
        key_shift, key_pos = jax.random.split(lane_keys[lane])
        layout = values.reshape(TOK_DEV, homes).T
        shift = jax.random.randint(key_shift, (), 0, homes)
        layout = jnp.roll(layout, shift, axis=0)
        pos_keys = jax.random.split(key_pos, homes)
        orders = jax.vmap(lambda k: jax.random.permutation(k, TOK_DEV))(pos_keys)
        layout = jnp.take_along_axis(layout, orders.astype(jnp.int32), axis=1)
        picks = layout.reshape(TOKENS)
        columns.append(labels[lane][picks])
    return jnp.stack(columns, axis=1).astype(jnp.int32)


def levels(key, dims, shards, least, largest):
    factor_of, own = 1.0, jax.random.fold_in(key, 6)
    for position, shards_of in shards:
        steps = jnp.exp(jax.random.uniform(jax.random.fold_in(own, position), (shards_of,), jnp.float32, least / len(shards), largest / len(shards)))
        factor_of = factor_of * jnp.repeat(steps, dims[position] // shards_of).reshape([-1 if axis == position else 1 for axis in range(len(dims))])
    return factor_of


def bell_draw(rng, dims, scale, bound, pieces=(), kind=jnp.bfloat16):
    level = levels(rng, dims, pieces, -0.22, 0.18) if pieces else 1.0
    result = jax.random.normal(rng, dims, jnp.float32) * scale * level
    return jnp.minimum(jnp.maximum(result, -bound), bound).astype(kind)


def setup_inputs(seed: int = 0) -> dict:
    key_list = jax.random.split(jax.random.key(seed), 5)
    return {
        "tokens": bell_draw(key_list[0], (TOKENS, D), 1.0, 6.0, ((0, 16),), jnp.float32),
        "route_ids": draw_route_ids(jax.random.fold_in(key_list[4], 71), 0),
        "route_weights": jnp.clip(jnp.exp(math.log(1.0) - 2.9957323 * jax.random.uniform(key_list[2], (TOKENS, TOP), jnp.float32) ** levels(key_list[2], (TOKENS, TOP), ((0, 16),), -0.2, 0.2)), 0.05, 1.0),
        "expert_rows": bell_draw(key_list[3], (EXPERTS, CAP, D), 1.0, 6.0, ((0, 32),), jnp.float32),
    }


def reference(tokens, route_ids, route_weights, expert_rows):
    real = route_ids < EXPERTS
    group = jnp.where(real, route_ids // (EXPERTS // N_GRP), (route_ids - EXPERTS) // (ZEXP // N_GRP))
    chosen = (route_ids[:, :, None] == jnp.arange(EXPERTS, dtype=jnp.int32)[None, None, :]).astype(jnp.int32).sum(1)
    before = jnp.cumsum(chosen, axis=0) - chosen
    safe_expert = jnp.where(real, route_ids, 0).astype(jnp.int32)
    rank = jnp.take_along_axis(before, safe_expert, axis=1)
    safe_rank = jnp.where(real, rank, 0).astype(jnp.int32)
    partials = []
    for which in range(N_GRP):
        total = jnp.zeros((TOKENS, D), jnp.float32)
        for slot in range(TOP):
            rows = expert_rows[safe_expert[:, slot], safe_rank[:, slot]]
            value = jnp.where(real[:, slot][:, None], rows, tokens)
            factor = jnp.where(group[:, slot] == which, route_weights[:, slot], jnp.zeros_like(route_weights[:, slot]))
            total = total + factor[:, None] * value
        partials.append(total)
    combined = partials[0]
    for which in range(1, N_GRP):
        combined = combined + partials[which]
    return combined
```

```python
import functools

import jax
import jax.numpy as jnp
from jax import lax
from jax.experimental import pallas as pl
from jax.experimental.pallas import tpu as pltpu
from jax.sharding import PartitionSpec as P

MESH = pl.DeviceIdType.MESH
ORDERS = ((2, 0, 1, 3), (0, 2, 1, 3), (1, 3, 0, 2), (1, 3, 0, 2), (2, 0, 1, 3), (0, 1, 2, 3))


def relative(index, r):
    out, b = index, 0
    while r >> b:
        if (r >> b) & 1:
            out = out + (1 << b) * (1 - 2 * ((index // (1 << b)) % 2))
        b += 1
    return out


def fold_orders(count, parts):
    return [
        [b for b in ORDERS[p % len(ORDERS)] if b < count] + list(range(len(ORDERS[0]), count))
        for p in range(parts)
    ]


def arrival_order(orders, count):
    parts = len(orders)
    ready = [((p + 1) * 0.5, p, 0) for p in range(parts)]
    free = [0.0] * (count + 1)
    events = []
    while ready:
        start, p, s = min(ready)
        ready.remove((start, p, s))
        bit = orders[p][s]
        units = (1 << (count - 1 - s)) * 8.4 / parts
        end = max(start, free[bit]) + (2 * units if bit > 2 else units)
        free[bit] = end
        if bit > 2:
            free[2] = max(start, free[2]) + units
            end = max(end, free[2])
        events.append((end, p, s))
        if s < count - 1:
            ready.append((end + 2.5, p, s + 1))
    return [(p, s) for _, p, s in sorted(events)]


def gather_kernel(count, groups, x_ref, e_ref, o_ref, *rest):
    swapped = rest[:groups - 1]
    send_sem, recv_sem, swap_send, swap_recv = rest[groups - 1:]
    n = 1 << count
    me, grp = lax.axis_index("ep"), lax.axis_index("grp")
    half = e_ref.shape[2] // groups
    peers = [relative(me, r) for r in range(n)]
    barrier = pltpu.get_barrier_semaphore()
    others = [lax.rem(grp + d, groups) for d in range(1, groups)]
    for g in others:
        pl.semaphore_signal(barrier, inc=1, device_id={"grp": g}, device_id_type=MESH)
    for r in range(1, n):
        pl.semaphore_signal(barrier, inc=1, device_id={"ep": peers[r]}, device_id_type=MESH)
    pl.semaphore_wait(barrier, n - 1 + groups - 1)
    copies = []
    for r in range(n - 1, 0, -1):
        copies.append(pltpu.make_async_remote_copy(
            src_ref=x_ref,
            dst_ref=o_ref.at[r],
            send_sem=send_sem.at[r],
            recv_sem=recv_sem.at[r],
            device_id={"ep": peers[r]},
            device_id_type=MESH,
        ))
    for d, g in enumerate(others):
        copies.append(pltpu.make_async_remote_copy(
            src_ref=e_ref.at[:, :, pl.ds(pl.multiple_of(g * half, 128), half)],
            dst_ref=swapped[d],
            send_sem=swap_send.at[d],
            recv_sem=swap_recv.at[d],
            device_id={"grp": g},
            device_id_type=MESH,
        ))
    for copy in copies:
        copy.start()
    o_ref[0] = x_ref[...]
    for copy in copies:
        copy.wait()


def gather_small(x, expert_rows, count, groups):
    n = 1 << count
    exp_dev, capacity, width = expert_rows.shape
    swap = jax.ShapeDtypeStruct((exp_dev, capacity, width // groups), expert_rows.dtype)
    vmem, anywhere = pl.BlockSpec(memory_space=pltpu.VMEM), pl.BlockSpec(memory_space=pl.ANY)
    return pl.pallas_call(
        functools.partial(gather_kernel, count, groups),
        out_shape=[jax.ShapeDtypeStruct((n,) + x.shape, x.dtype)] + [swap] * (groups - 1),
        in_specs=[vmem, anywhere],
        out_specs=[vmem] + [anywhere] * (groups - 1),
        scratch_shapes=[
            pltpu.SemaphoreType.DMA((n,)),
            pltpu.SemaphoreType.DMA((n,)),
            pltpu.SemaphoreType.DMA((groups - 1,)),
            pltpu.SemaphoreType.DMA((groups - 1,)),
        ],
        compiler_params=pltpu.CompilerParams(collective_id=0, has_side_effects=True),
    )(x, expert_rows)


def scatter_kernel(count, parts, groups, column, c_ref, e_ref, *rest):
    swapped = rest[:groups - 1]
    o_ref, rows, acc, got, load_sem, send_sem, recv_sem = rest[groups - 1:]
    n = 1 << count
    tok = c_ref.shape[1]
    exp_dev, capacity, width = e_ref.shape
    half_width = width // groups
    wide = acc.shape[2]
    me, grp = lax.axis_index("ep"), lax.axis_index("grp")

    def loads(p):
        out = []
        start = column + p * wide
        for i in range(groups * exp_dev):
            g, e = i // exp_dev, i % exp_dev
            if g == 0:
                src = e_ref.at[e, :, pl.ds(pl.multiple_of(grp * half_width + start, 128), wide)]
            else:
                src = swapped[g - 1].at[e, :, pl.ds(start, wide)]
            dst = rows.at[p, pl.ds(i * capacity, capacity)]
            out.append(pltpu.make_async_copy(src, dst, load_sem.at[p, i]))
        return out

    loading = [loads(p) for p in range(parts)]
    for p in range(parts):
        for copy in loading[p]:
            copy.start()

    peers = [relative(me, 1 << b) for b in range(count)]
    barrier = pltpu.get_barrier_semaphore()
    for b in range(count):
        pl.semaphore_signal(barrier, inc=1, device_id={"ep": peers[b]}, device_id_type=MESH)
    orders = fold_orders(count, parts)

    def place(p, q):
        return sum(((q >> (count - 1 - s)) & 1) << orders[p][s] for s in range(count))

    def multiply(p, low, high):
        weights = jnp.concatenate([c_ref[place(p, q)] for q in range(low, high)], axis=0)
        acc[p, low * tok:high * tok, :] = jnp.dot(
            weights,
            rows[p],
            preferred_element_type=jnp.float32,
            precision=lax.Precision.HIGHEST,
        )

    def transfer(p, s):
        half = (n >> (s + 1)) * tok
        return pltpu.make_async_remote_copy(
            src_ref=acc.at[p, pl.ds(half, half)],
            dst_ref=got.at[p, pl.ds(half, half)],
            send_sem=send_sem.at[p, s],
            recv_sem=recv_sem.at[p, s],
            device_id={"ep": peers[orders[p][s]]},
            device_id_type=MESH,
        )

    copies = [[transfer(p, s) for s in range(count)] for p in range(parts)]
    for p in range(parts):
        for copy in loading[p]:
            copy.wait()
        multiply(p, n // 2, n)
        if p == 0:
            pl.semaphore_wait(barrier, count)
        copies[p][0].start()
    for p in range(parts):
        multiply(p, 0, n // 2)
    for p, s in arrival_order(orders, count):
        half = (n >> (s + 1)) * tok
        copies[p][s].wait_recv()
        if s < count - 1:
            mid = half // 2
            acc[p, mid:half, :] += got[p, half + mid:2 * half, :]
            copies[p][s + 1].start()
            acc[p, 0:mid, :] += got[p, half:half + mid, :]
        else:
            o_ref[:, p * wide:(p + 1) * wide] = acc[p, 0:tok, :] + got[p, tok:2 * tok, :]
    for p in range(parts):
        for s in range(count):
            copies[p][s].wait_send()


def scatter_sum(c, expert_rows, swapped, count, parts, column, span):
    n, tok, depth = c.shape
    groups = len(swapped) + 1
    wide = span // parts
    vmem, anywhere = pl.BlockSpec(memory_space=pltpu.VMEM), pl.BlockSpec(memory_space=pl.ANY)
    return pl.pallas_call(
        functools.partial(scatter_kernel, count, parts, groups, column),
        out_shape=jax.ShapeDtypeStruct((tok, span), jnp.float32),
        in_specs=[vmem, anywhere] + [anywhere] * (groups - 1),
        out_specs=vmem,
        scratch_shapes=[
            pltpu.VMEM((parts, depth, wide), jnp.float32),
            pltpu.VMEM((parts, n * tok, wide), jnp.float32),
            pltpu.VMEM((parts, n * tok, wide), jnp.float32),
            pltpu.SemaphoreType.DMA((parts, groups * expert_rows.shape[0])),
            pltpu.SemaphoreType.DMA((parts, count)),
            pltpu.SemaphoreType.DMA((parts, count)),
        ],
        compiler_params=pltpu.CompilerParams(
            collective_id=1, has_side_effects=True, vmem_limit_bytes=60 << 20
        ),
    )(c, expert_rows, *swapped)

FOLD_PARTS = 12
FOLD_ORDERS = {
    (4, 12): (
        (0, 2, 3, 1), (1, 0, 2, 3), (2, 1, 0, 3), (2, 1, 0, 3), (1, 3, 2, 0), (1, 2, 0, 3),
        (0, 1, 2, 3), (0, 1, 2, 3), (1, 0, 2, 3), (2, 0, 3, 1), (0, 2, 1, 3), (1, 0, 2, 3),
    ),
}
FOLD_SEQUENCE = {
    (4, 12): (
        (0, 0), (1, 0), (2, 0), (6, 0), (4, 0), (3, 0), (7, 0), (5, 0), (9, 0), (10, 0), (8, 0), (0, 1),
        (4, 1), (1, 1), (5, 1), (9, 1), (11, 0), (10, 1), (8, 1), (0, 2), (2, 1), (5, 2), (4, 2), (6, 1),
        (1, 2), (11, 1), (9, 2), (8, 2), (2, 2), (3, 1), (4, 3), (5, 3), (6, 2), (7, 1), (1, 3), (11, 2),
        (3, 2), (10, 2), (0, 3), (9, 3), (2, 3), (8, 3), (7, 2), (6, 3), (3, 3), (10, 3), (11, 3), (7, 3),
    ),
}


def fused_kernel(count, parts, groups, experts, t_ref, i_ref, w_ref, e_ref, o_ref, ids_own, w_own, ids_all, w_all,
                 own, rows, lower, flat, table, acc, got, small_sem, load_sem, gather_send, gather_recv,
                 swap_send, swap_recv, send_sem, recv_sem):
    n = 1 << count
    top, tok = i_ref.shape
    exp_dev, capacity, width = e_ref.shape
    half_width = width // groups
    wide = half_width // parts
    me, grp = lax.axis_index("ep"), lax.axis_index("grp")
    peers = [relative(me, r) for r in range(n)]
    others = [lax.rem(grp + d, groups) for d in range(1, groups)]

    smalls = [
        pltpu.make_async_copy(i_ref, ids_own, small_sem.at[0]),
        pltpu.make_async_copy(w_ref, w_own, small_sem.at[1]),
        pltpu.make_async_copy(
            t_ref.at[:, pl.ds(pl.multiple_of(grp * half_width, 128), half_width)], own, small_sem.at[2]
        ),
    ]
    for copy in smalls:
        copy.start()
    barrier = pltpu.get_barrier_semaphore()
    for r in range(1, n):
        pl.semaphore_signal(barrier, inc=1, device_id={"ep": peers[r]}, device_id_type=MESH)
    for g in others:
        pl.semaphore_signal(barrier, inc=1, device_id={"grp": g}, device_id_type=MESH)

    def columns(g, p):
        return pl.ds(pl.multiple_of(g * half_width + p * wide, 128), wide)

    loads = [
        [
            pltpu.make_async_copy(
                e_ref.at[e, :, columns(grp, p)], rows.at[p, pl.ds(e * capacity, capacity)], load_sem.at[p, e]
            )
            for e in range(exp_dev)
        ]
        for p in range(parts)
    ]
    for p in range(parts):
        for copy in loads[p]:
            copy.start()

    block = n * tok
    across = jnp.concatenate(
        [lax.broadcasted_iota(jnp.int32, (1, tok), 1) + peers[r] * tok for r in range(n)], axis=1
    )
    down = jnp.concatenate(
        [lax.broadcasted_iota(jnp.int32, (tok, 1), 0) + peers[r] * tok for r in range(n)], axis=0
    )
    lower[...] = jnp.where(down < across, 1.0, 0.0).astype(lower.dtype)

    smalls[0].wait()
    smalls[1].wait()
    pl.semaphore_wait(barrier, n - 1 + groups - 1)
    gathers = []
    for r in range(n - 1, 0, -1):
        for k, (src, dst) in enumerate(((ids_own, ids_all), (w_own, w_all))):
            gathers.append(pltpu.make_async_remote_copy(
                src_ref=src,
                dst_ref=dst.at[r],
                send_sem=gather_send.at[k, r],
                recv_sem=gather_recv.at[k, r],
                device_id={"ep": peers[r]},
                device_id_type=MESH,
            ))
    for copy in gathers:
        copy.start()
    swaps = [
        [
            pltpu.make_async_remote_copy(
                src_ref=e_ref.at[e, :, columns(g, p)],
                dst_ref=rows.at[p, pl.ds(((d + 1) * exp_dev + e) * capacity, capacity)],
                send_sem=swap_send.at[p, d, e],
                recv_sem=swap_recv.at[p, d, e],
                device_id={"grp": g},
                device_id_type=MESH,
            )
            for d, g in enumerate(others) for e in range(exp_dev)
        ]
        for p in range(parts)
    ]
    for p in range(parts):
        for copy in swaps[p]:
            copy.start()

    chosen = ids_own[...]
    ident_row = jnp.sum(jnp.where(chosen >= experts, w_own[...], 0.0), axis=0, keepdims=True)
    eye = lax.broadcasted_iota(jnp.int32, (tok, tok), 0) == lax.broadcasted_iota(jnp.int32, (tok, tok), 1)
    ident = jnp.sum(jnp.where(eye, ident_row, 0.0), axis=1, keepdims=True)
    smalls[2].wait()

    for copy in gathers:
        copy.wait()
    ids = jnp.concatenate([chosen] + [ids_all[r] for r in range(1, n)], axis=1)
    weights = jnp.concatenate([w_own[...]] + [w_all[r] for r in range(1, n)], axis=1)
    hits, picked = [], []
    for d in range(groups):
        for e in range(exp_dev):
            expert = (lax.rem(grp + groups - d, groups) * n + me) * exp_dev + e
            match = ids == expert
            hits.append(jnp.sum(jnp.where(match, 1.0, 0.0), axis=0, keepdims=True))
            picked.append(jnp.sum(jnp.where(match, weights, 0.0), axis=0, keepdims=True))
    hit = jnp.concatenate(hits, axis=0)
    rank = jnp.dot(hit.astype(lower.dtype), lower[...], preferred_element_type=jnp.float32)
    slot = jnp.where(hit > 0.0, rank, -1.0)
    level = lax.broadcasted_iota(jnp.int32, (capacity, block), 0).astype(jnp.float32)
    for j in range(groups * exp_dev):
        flat[j * capacity:(j + 1) * capacity, :] = jnp.where(level == slot[j:j + 1, :], picked[j], 0.0)
    table[...] = jnp.transpose(flat[...])

    orders = fold_table(count, parts)

    def place(p, q):
        return sum(((q >> (count - 1 - s)) & 1) << orders[p][s] for s in range(count))

    def multiply(p, low, high):
        spots = [place(p, q) for q in range(low, high)]
        left = jnp.concatenate([table[x * tok:(x + 1) * tok, :] for x in spots], axis=0)
        product = jnp.dot(left, rows[p], preferred_element_type=jnp.float32, precision=lax.Precision.HIGHEST)
        acc[p, low * tok:high * tok, :] = product
        if low == 0:
            acc[p, 0:tok, :] += ident * own[:, p * wide:(p + 1) * wide]

    def transfer(p, s):
        size = (n >> (s + 1)) * tok
        return pltpu.make_async_remote_copy(
            src_ref=acc.at[p, pl.ds(size, size)],
            dst_ref=got.at[p, pl.ds(size, size)],
            send_sem=send_sem.at[p, s],
            recv_sem=recv_sem.at[p, s],
            device_id={"ep": peers[1 << orders[p][s]]},
            device_id_type=MESH,
        )

    copies = [[transfer(p, s) for s in range(count)] for p in range(parts)]
    for p in range(parts):
        for copy in loads[p]:
            copy.wait()
        for copy in swaps[p]:
            copy.wait()
        multiply(p, n // 2, n)
        copies[p][0].start()
    for p in range(parts):
        multiply(p, 0, n // 2)
    for p, s in fold_sequence(count, parts):
        size = (n >> (s + 1)) * tok
        copies[p][s].wait_recv()
        if s < count - 1:
            mid = size // 2
            acc[p, mid:size, :] += got[p, size + mid:2 * size, :]
            copies[p][s + 1].start()
            acc[p, 0:mid, :] += got[p, size:size + mid, :]
        else:
            o_ref[:, p * wide:(p + 1) * wide] = acc[p, 0:tok, :] + got[p, tok:2 * tok, :]
    for p in range(parts):
        for s in range(count):
            copies[p][s].wait_send()


def fold_table(count, parts):
    return FOLD_ORDERS.get((count, parts)) or fold_orders(count, parts)


def fold_sequence(count, parts):
    return FOLD_SEQUENCE.get((count, parts)) or arrival_order(fold_orders(count, parts), count)


def fused_sizes(n, tok, exp_dev, capacity, width, groups):
    half = width // groups
    depth = groups * exp_dev * capacity
    floats = 2 * n * tok * half + depth * half + 2 * depth * n * tok + (n * tok) ** 2 // 2 + 2 * tok * half
    tiles = half // 128
    parts = max(d for d in range(1, tiles + 1) if tiles % d == 0 and d <= FOLD_PARTS)
    fits = floats * 4 <= (40 << 20) and n > 1 and depth % 128 == 0 and (n * tok) % 128 == 0 and tok % 8 == 0
    return parts, fits


def fused(tokens, route_ids, route_weights, expert_rows, count, parts, groups, experts):
    n = 1 << count
    tok, top = route_ids.shape
    exp_dev, capacity, width = expert_rows.shape
    half = width // groups
    wide = half // parts
    depth = groups * exp_dev * capacity
    anywhere = pl.BlockSpec(memory_space=pl.ANY)
    return pl.pallas_call(
        functools.partial(fused_kernel, count, parts, groups, experts),
        out_shape=jax.ShapeDtypeStruct((tok, half), jnp.float32),
        in_specs=[anywhere] * 4,
        out_specs=pl.BlockSpec(memory_space=pltpu.VMEM),
        scratch_shapes=[
            pltpu.VMEM((top, tok), jnp.int32),
            pltpu.VMEM((top, tok), jnp.float32),
            pltpu.VMEM((n, top, tok), jnp.int32),
            pltpu.VMEM((n, top, tok), jnp.float32),
            pltpu.VMEM((tok, half), jnp.float32),
            pltpu.VMEM((parts, depth, wide), jnp.float32),
            pltpu.VMEM((n * tok, n * tok), jnp.bfloat16),
            pltpu.VMEM((depth, n * tok), jnp.float32),
            pltpu.VMEM((n * tok, depth), jnp.float32),
            pltpu.VMEM((parts, n * tok, wide), jnp.float32),
            pltpu.VMEM((parts, n * tok, wide), jnp.float32),
            pltpu.SemaphoreType.DMA((3,)),
            pltpu.SemaphoreType.DMA((parts, exp_dev)),
            pltpu.SemaphoreType.DMA((2, n)),
            pltpu.SemaphoreType.DMA((2, n)),
            pltpu.SemaphoreType.DMA((parts, groups - 1, exp_dev)),
            pltpu.SemaphoreType.DMA((parts, groups - 1, exp_dev)),
            pltpu.SemaphoreType.DMA((parts, count)),
            pltpu.SemaphoreType.DMA((parts, count)),
        ],
        compiler_params=pltpu.CompilerParams(
            collective_id=2, has_side_effects=True, vmem_limit_bytes=60 << 20
        ),
    )(tokens, route_ids.T, route_weights.T, expert_rows)


def shards(tokens, route_ids, route_weights, expert_rows):
    groups = lax.axis_size("grp")
    n = lax.axis_size("ep")
    count = n.bit_length() - 1
    group_index = lax.axis_index("grp")
    ep_index = lax.axis_index("ep")
    exp_dev, capacity, width = expert_rows.shape
    tok, top = route_ids.shape
    experts = exp_dev * groups * n
    half = width // groups
    depth = exp_dev * groups * capacity
    parts, fits = fused_sizes(n, tok, exp_dev, capacity, width, groups)
    if fits:
        return fused(tokens, route_ids, route_weights, expert_rows, count, parts, groups, experts)

    packed = jnp.concatenate([route_ids.astype(jnp.float32), route_weights], axis=1)
    lanes = 128 if packed.size % 128 == 0 else packed.shape[1]
    everyone, *swapped = gather_small(packed.reshape(-1, lanes), expert_rows, count, groups)
    everyone = everyone.reshape((n,) + packed.shape)
    owners = [(group_index - d) % groups for d in range(groups)]
    owned = [(g * n + ep_index) * exp_dev + j for g in owners for j in range(exp_dev)]

    ids = everyone[:, :, :top].astype(jnp.int32)
    weights = everyone[:, :, top:]
    homes = jnp.stack([relative(ep_index, r) for r in range(n)])
    earlier_home = (homes[None, :] < homes[:, None]).astype(jnp.float32)
    lower = (jnp.arange(tok)[None, :] < jnp.arange(tok)[:, None]).astype(jnp.float32)
    lane = lax.broadcasted_iota(jnp.int32, (n, tok, depth), 2)
    table = jnp.zeros((n, tok, depth), jnp.float32)
    for j, expert in enumerate(owned):
        match = ids == expert
        hit = jnp.sum(match.astype(jnp.float32), axis=2)
        weight = jnp.sum(jnp.where(match, weights, 0.0), axis=2)
        before = jnp.sum(earlier_home * jnp.sum(hit, axis=1)[None, :], axis=1)
        within = jnp.sum(lower[None, :, :] * hit[:, None, :], axis=2)
        rank = (before[:, None] + within).astype(jnp.int32)
        slot = jnp.where(hit > 0, jnp.minimum(rank, capacity - 1) + j * capacity, -1)
        table = table + jnp.where(lane == slot[:, :, None], weight[:, :, None], 0.0)

    tiles = half // 128
    fits = max(1, (8 << 20) // (n * tok * 128 * 4))
    chunk = max(d for d in range(1, tiles + 1) if tiles % d == 0 and d <= fits)
    parts = max(d for d in range(1, chunk + 1) if chunk % d == 0 and d <= len(ORDERS))
    sums = [
        scatter_sum(table, expert_rows, swapped, count, parts, a * 128, chunk * 128)
        for a in range(0, tiles, chunk)
    ]
    total = sums[0] if len(sums) == 1 else jnp.concatenate(sums, axis=1)
    ident = jnp.sum(jnp.where(route_ids >= experts, route_weights, 0.0), axis=1)
    own_half = lax.dynamic_slice_in_dim(tokens, group_index * half, half, 1)
    return total + ident[:, None] * own_half


def solution(mesh):
    placed = (P("ep", None), P("ep", None), P("ep", None), P(("grp", "ep"), None, None))
    return jax.shard_map(
        shards, mesh=mesh, in_specs=placed, out_specs=P("ep", "grp"), check_vma=False
    )
```

```python
import functools

import jax
import jax.numpy as jnp
from jax import lax
from jax.experimental import pallas as pl
from jax.experimental.pallas import tpu as pltpu
from jax.sharding import PartitionSpec as P

MESH = pl.DeviceIdType.MESH
ORDERS = ((2, 0, 1, 3), (0, 2, 1, 3), (1, 3, 0, 2), (1, 3, 0, 2), (2, 0, 1, 3), (0, 1, 2, 3))


def relative(index, r):
    out, b = index, 0
    while r >> b:
        if (r >> b) & 1:
            out = out + (1 << b) * (1 - 2 * ((index // (1 << b)) % 2))
        b += 1
    return out


def fold_orders(count, parts):
    return [
        [b for b in ORDERS[p % len(ORDERS)] if b < count] + list(range(len(ORDERS[0]), count))
        for p in range(parts)
    ]


def arrival_order(orders, count):
    parts = len(orders)
    ready = [((p + 1) * 0.5, p, 0) for p in range(parts)]
    free = [0.0] * (count + 1)
    events = []
    while ready:
        start, p, s = min(ready)
        ready.remove((start, p, s))
        bit = orders[p][s]
        units = (1 << (count - 1 - s)) * 8.4 / parts
        end = max(start, free[bit]) + (2 * units if bit > 2 else units)
        free[bit] = end
        if bit > 2:
            free[2] = max(start, free[2]) + units
            end = max(end, free[2])
        events.append((end, p, s))
        if s < count - 1:
            ready.append((end + 2.5, p, s + 1))
    return [(p, s) for _, p, s in sorted(events)]


def gather_kernel(count, groups, x_ref, e_ref, o_ref, *rest):
    swapped = rest[:groups - 1]
    send_sem, recv_sem, swap_send, swap_recv = rest[groups - 1:]
    n = 1 << count
    me, grp = lax.axis_index("ep"), lax.axis_index("grp")
    half = e_ref.shape[2] // groups
    peers = [relative(me, r) for r in range(n)]
    barrier = pltpu.get_barrier_semaphore()
    others = [lax.rem(grp + d, groups) for d in range(1, groups)]
    for g in others:
        pl.semaphore_signal(barrier, inc=1, device_id={"grp": g}, device_id_type=MESH)
    for r in range(1, n):
        pl.semaphore_signal(barrier, inc=1, device_id={"ep": peers[r]}, device_id_type=MESH)
    pl.semaphore_wait(barrier, n - 1 + groups - 1)
    copies = []
    for r in range(n - 1, 0, -1):
        copies.append(pltpu.make_async_remote_copy(
            src_ref=x_ref,
            dst_ref=o_ref.at[r],
            send_sem=send_sem.at[r],
            recv_sem=recv_sem.at[r],
            device_id={"ep": peers[r]},
            device_id_type=MESH,
        ))
    for d, g in enumerate(others):
        copies.append(pltpu.make_async_remote_copy(
            src_ref=e_ref.at[:, :, pl.ds(pl.multiple_of(g * half, 128), half)],
            dst_ref=swapped[d],
            send_sem=swap_send.at[d],
            recv_sem=swap_recv.at[d],
            device_id={"grp": g},
            device_id_type=MESH,
        ))
    for copy in copies:
        copy.start()
    o_ref[0] = x_ref[...]
    for copy in copies:
        copy.wait()


def gather_small(x, expert_rows, count, groups):
    n = 1 << count
    exp_dev, capacity, width = expert_rows.shape
    swap = jax.ShapeDtypeStruct((exp_dev, capacity, width // groups), expert_rows.dtype)
    vmem, anywhere = pl.BlockSpec(memory_space=pltpu.VMEM), pl.BlockSpec(memory_space=pl.ANY)
    return pl.pallas_call(
        functools.partial(gather_kernel, count, groups),
        out_shape=[jax.ShapeDtypeStruct((n,) + x.shape, x.dtype)] + [swap] * (groups - 1),
        in_specs=[vmem, anywhere],
        out_specs=[vmem] + [anywhere] * (groups - 1),
        scratch_shapes=[
            pltpu.SemaphoreType.DMA((n,)),
            pltpu.SemaphoreType.DMA((n,)),
            pltpu.SemaphoreType.DMA((groups - 1,)),
            pltpu.SemaphoreType.DMA((groups - 1,)),
        ],
        compiler_params=pltpu.CompilerParams(collective_id=0, has_side_effects=True),
    )(x, expert_rows)


def scatter_kernel(count, parts, groups, column, c_ref, e_ref, *rest):
    swapped = rest[:groups - 1]
    o_ref, rows, acc, got, load_sem, send_sem, recv_sem = rest[groups - 1:]
    n = 1 << count
    tok = c_ref.shape[1]
    exp_dev, capacity, width = e_ref.shape
    half_width = width // groups
    wide = acc.shape[2]
    me, grp = lax.axis_index("ep"), lax.axis_index("grp")

    def loads(p):
        out = []
        start = column + p * wide
        for i in range(groups * exp_dev):
            g, e = i // exp_dev, i % exp_dev
            if g == 0:
                src = e_ref.at[e, :, pl.ds(pl.multiple_of(grp * half_width + start, 128), wide)]
            else:
                src = swapped[g - 1].at[e, :, pl.ds(start, wide)]
            dst = rows.at[p, pl.ds(i * capacity, capacity)]
            out.append(pltpu.make_async_copy(src, dst, load_sem.at[p, i]))
        return out

    loading = [loads(p) for p in range(parts)]
    for p in range(parts):
        for copy in loading[p]:
            copy.start()

    peers = [relative(me, 1 << b) for b in range(count)]
    barrier = pltpu.get_barrier_semaphore()
    for b in range(count):
        pl.semaphore_signal(barrier, inc=1, device_id={"ep": peers[b]}, device_id_type=MESH)
    orders = fold_orders(count, parts)

    def place(p, q):
        return sum(((q >> (count - 1 - s)) & 1) << orders[p][s] for s in range(count))

    def multiply(p, low, high):
        weights = jnp.concatenate([c_ref[place(p, q)] for q in range(low, high)], axis=0)
        acc[p, low * tok:high * tok, :] = jnp.dot(
            weights,
            rows[p],
            preferred_element_type=jnp.float32,
            precision=lax.Precision.HIGHEST,
        )

    def transfer(p, s):
        half = (n >> (s + 1)) * tok
        return pltpu.make_async_remote_copy(
            src_ref=acc.at[p, pl.ds(half, half)],
            dst_ref=got.at[p, pl.ds(half, half)],
            send_sem=send_sem.at[p, s],
            recv_sem=recv_sem.at[p, s],
            device_id={"ep": peers[orders[p][s]]},
            device_id_type=MESH,
        )

    copies = [[transfer(p, s) for s in range(count)] for p in range(parts)]
    for p in range(parts):
        for copy in loading[p]:
            copy.wait()
        multiply(p, n // 2, n)
        if p == 0:
            pl.semaphore_wait(barrier, count)
        copies[p][0].start()
    for p in range(parts):
        multiply(p, 0, n // 2)
    for p, s in arrival_order(orders, count):
        half = (n >> (s + 1)) * tok
        copies[p][s].wait_recv()
        if s < count - 1:
            mid = half // 2
            acc[p, mid:half, :] += got[p, half + mid:2 * half, :]
            copies[p][s + 1].start()
            acc[p, 0:mid, :] += got[p, half:half + mid, :]
        else:
            o_ref[:, p * wide:(p + 1) * wide] = acc[p, 0:tok, :] + got[p, tok:2 * tok, :]
    for p in range(parts):
        for s in range(count):
            copies[p][s].wait_send()


def scatter_sum(c, expert_rows, swapped, count, parts, column, span):
    n, tok, depth = c.shape
    groups = len(swapped) + 1
    wide = span // parts
    vmem, anywhere = pl.BlockSpec(memory_space=pltpu.VMEM), pl.BlockSpec(memory_space=pl.ANY)
    return pl.pallas_call(
        functools.partial(scatter_kernel, count, parts, groups, column),
        out_shape=jax.ShapeDtypeStruct((tok, span), jnp.float32),
        in_specs=[vmem, anywhere] + [anywhere] * (groups - 1),
        out_specs=vmem,
        scratch_shapes=[
            pltpu.VMEM((parts, depth, wide), jnp.float32),
            pltpu.VMEM((parts, n * tok, wide), jnp.float32),
            pltpu.VMEM((parts, n * tok, wide), jnp.float32),
            pltpu.SemaphoreType.DMA((parts, groups * expert_rows.shape[0])),
            pltpu.SemaphoreType.DMA((parts, count)),
            pltpu.SemaphoreType.DMA((parts, count)),
        ],
        compiler_params=pltpu.CompilerParams(
            collective_id=1, has_side_effects=True, vmem_limit_bytes=60 << 20
        ),
    )(c, expert_rows, *swapped)


PARTS = 6
FUSED_COUNT = 4
FUSED_ORDERS = (
        (2, 1, 3, 0), (0, 1, 2, 3), (1, 2, 0, 3), (2, 0, 1, 3), (0, 1, 2, 3), (0, 1, 2, 3),
)
FUSED_SEQUENCE = (
        (0, 0, 0), (1, 0, 0), (2, 0, 0), (0, 1, 0), (0, 1, 1), (3, 0, 0), (4, 0, 0), (1, 1, 0), (2, 1, 0), (1, 1, 1),
        (0, 2, 0), (2, 1, 1), (4, 1, 0), (5, 0, 0), (0, 2, 1), (1, 2, 0), (3, 1, 0), (1, 2, 1), (4, 1, 1), (4, 2, 0),
        (3, 1, 1), (5, 1, 0), (4, 2, 1), (1, 3, 0), (2, 2, 0), (5, 1, 1), (0, 3, 0), (1, 3, 1), (0, 3, 1), (2, 2, 1),
        (3, 2, 0), (1, 4, 0), (4, 3, 0), (3, 2, 1), (4, 3, 1), (5, 2, 0), (4, 4, 0), (5, 2, 1), (0, 4, 0), (2, 3, 0),
        (2, 3, 1), (3, 3, 0), (2, 4, 0), (3, 3, 1), (5, 3, 0), (5, 3, 1), (3, 4, 0), (5, 4, 0),
)


def fused_kernel(count, groups, experts, firsts, t_ref, i_ref, w_ref, e_ref, o_ref, ids_own, w_own, ids_all, w_all,
                 own, rows, lower, flat, table, acc, got, last, small_sem, load_sem, gather_send, gather_recv,
                 swap_send, swap_recv, fold_send, fold_recv, last_send, last_recv):
    n = 1 << count
    top, tok = i_ref.shape
    exp_dev, capacity, width = e_ref.shape
    half_width = width // groups
    wide = acc.shape[2]
    parts = acc.shape[0]
    depth = groups * exp_dev * capacity
    orders = FUSED_ORDERS
    me, grp = lax.axis_index("ep"), lax.axis_index("grp")
    peers = [relative(me, r) for r in range(n)]
    others = [lax.rem(grp + d, groups) for d in range(1, groups)]
    sides = [lax.rem(me // (1 << orders[p][0]), 2) for p in range(parts)]

    def mine(p):
        return pl.ds(pl.multiple_of(2 * p * wide + sides[p] * wide, 128), wide)

    def theirs(p):
        return pl.ds(pl.multiple_of(2 * p * wide + (1 - sides[p]) * wide, 128), wide)

    def source(g, p, side):
        return e_ref.at[:, :, pl.ds(pl.multiple_of(g * half_width + 2 * p * wide + side * wide, 128), wide)]

    smalls = [
        pltpu.make_async_copy(i_ref, ids_own, small_sem.at[0]),
        pltpu.make_async_copy(w_ref, w_own, small_sem.at[1]),
        pltpu.make_async_copy(
            t_ref.at[:, pl.ds(pl.multiple_of(grp * half_width, 128), half_width)], own, small_sem.at[2]
        ),
    ]
    for copy in smalls:
        copy.start()
    barrier = pltpu.get_barrier_semaphore()
    for r in range(n - 1, 0, -1):
        pl.semaphore_signal(barrier, inc=1, device_id={"ep": peers[r]}, device_id_type=MESH)
    for g in others:
        for b in firsts:
            pl.semaphore_signal(barrier, inc=1, device_id={"grp": g, "ep": peers[1 << b]}, device_id_type=MESH)
        pl.semaphore_signal(barrier, inc=1, device_id={"grp": g}, device_id_type=MESH)

    loads = [pltpu.make_async_copy(source(grp, p, sides[p]), rows.at[p, 0], load_sem.at[p]) for p in range(parts)]
    for copy in loads:
        copy.start()

    block = n * tok
    across = jnp.concatenate(
        [lax.broadcasted_iota(jnp.int32, (1, tok), 1) + peers[r] * tok for r in range(n)], axis=1
    )
    down = jnp.concatenate(
        [lax.broadcasted_iota(jnp.int32, (tok, 1), 0) + peers[r] * tok for r in range(n)], axis=0
    )
    lower[...] = jnp.where(down < across, 1.0, 0.0).astype(lower.dtype)

    smalls[0].wait()
    smalls[1].wait()
    pl.semaphore_wait(barrier, n - 1 + (groups - 1) * (1 + len(firsts)))
    gathers = []
    for r in range(n - 1, 0, -1):
        for k, (src, dst) in enumerate(((ids_own, ids_all), (w_own, w_all))):
            gathers.append(pltpu.make_async_remote_copy(
                src_ref=src,
                dst_ref=dst.at[r],
                send_sem=gather_send.at[k, r],
                recv_sem=gather_recv.at[k, r],
                device_id={"ep": peers[r]},
                device_id_type=MESH,
            ))
    for copy in gathers:
        copy.start()

    def swap(p, slot):
        c, d = slot // groups, slot % groups
        to = {}
        if c:
            to["ep"] = peers[1 << orders[p][0]]
        if d:
            to["grp"] = others[d - 1]
        return pltpu.make_async_remote_copy(
            src_ref=source(lax.rem(grp + d, groups), p, 1 - sides[p] if c else sides[p]),
            dst_ref=rows.at[p, slot],
            send_sem=swap_send.at[p, slot],
            recv_sem=swap_recv.at[p, slot],
            device_id=to,
            device_id_type=MESH,
        )

    swaps = [[swap(p, slot) for slot in range(2 * groups - 1, 0, -1)] for p in range(parts)]
    for p in range(parts):
        for copy in swaps[p]:
            copy.start()

    chosen = ids_own[...]
    ident_row = jnp.sum(jnp.where(chosen >= experts, w_own[...], 0.0), axis=0, keepdims=True)
    eye = lax.broadcasted_iota(jnp.int32, (tok, tok), 0) == lax.broadcasted_iota(jnp.int32, (tok, tok), 1)
    ident = jnp.sum(jnp.where(eye, ident_row, 0.0), axis=1, keepdims=True)
    smalls[2].wait()

    for copy in gathers:
        copy.wait_recv()
    ids = jnp.concatenate([chosen] + [ids_all[r] for r in range(1, n)], axis=1)
    weights = jnp.concatenate([w_own[...]] + [w_all[r] for r in range(1, n)], axis=1)
    chips = [me] + [peers[1 << b] for b in firsts]
    hits, picked = [], []
    for chip in chips:
        for d in range(groups):
            for e in range(exp_dev):
                expert = (lax.rem(grp + groups - d, groups) * n + chip) * exp_dev + e
                match = ids == expert
                hits.append(jnp.sum(jnp.where(match, 1.0, 0.0), axis=0, keepdims=True))
                picked.append(jnp.sum(jnp.where(match, weights, 0.0), axis=0, keepdims=True))
    hit = jnp.concatenate(hits, axis=0)
    rank = jnp.dot(hit.astype(lower.dtype), lower[...], preferred_element_type=jnp.float32)
    slots = jnp.where(hit > 0.0, rank, -1.0)
    level = lax.broadcasted_iota(jnp.int32, (capacity, block), 0).astype(jnp.float32)
    each = groups * exp_dev
    for c in range(len(chips)):
        for j in range(each):
            i = c * each + j
            flat[c, j * capacity:(j + 1) * capacity, :] = jnp.where(level == slots[i:i + 1, :], picked[i], 0.0)
        table[c] = jnp.transpose(flat[c])

    def place(p, q):
        out = (q % 2) << orders[p][0]
        return out + sum(((q >> (count - k)) & 1) << orders[p][k] for k in range(1, count))

    def multiply(p, low, high):
        c = 1 + firsts.index(orders[p][0])
        spots = [pl.ds(place(p, q) * tok, tok) for q in range(low, high)]
        left = jnp.concatenate(
            [jnp.concatenate([table[x, spot, :] for spot in spots], axis=0) for x in (0, c)], axis=1
        )
        acc[p, low * tok:high * tok, :] = jnp.dot(
            left,
            rows[p].reshape(2 * depth, wide),
            preferred_element_type=jnp.float32,
            precision=lax.Precision.HIGHEST,
        )

    def fold(p, k, h):
        size = (n >> k) * tok
        mid = size // 2
        where = pl.ds(size + mid if h == 0 else size, mid)
        return pltpu.make_async_remote_copy(
            src_ref=acc.at[p, where],
            dst_ref=got.at[p, where],
            send_sem=fold_send.at[p, k - 1, h],
            recv_sem=fold_recv.at[p, k - 1, h],
            device_id={"ep": peers[1 << orders[p][k]]},
            device_id_type=MESH,
        )

    folds = {(p, k, h): fold(p, k, h) for p in range(parts) for k in range(1, count) for h in range(2)}
    lasts = [
        pltpu.make_async_remote_copy(
            src_ref=acc.at[p, pl.ds(tok, tok)],
            dst_ref=last.at[p],
            send_sem=last_send.at[p],
            recv_sem=last_recv.at[p],
            device_id={"ep": peers[1 << orders[p][0]]},
            device_id_type=MESH,
        )
        for p in range(parts)
    ]

    def add(p, size, low, high):
        acc[p, low:high, :] += got[p, size + low:size + high, :]

    for p, k, h in FUSED_SEQUENCE:
        size = (n >> k) * tok
        mid = size // 2
        if k == 0:
            loads[p].wait()
            for copy in swaps[p]:
                copy.wait_recv()
            multiply(p, n // 2, n)
            folds[p, 1, 0].start()
            folds[p, 1, 1].start()
            multiply(p, 0, n // 2)
        elif k < count - 1:
            folds[p, k, h].wait_recv()
            if h == 0:
                for half in range(2):
                    low = mid + mid // 2 if half == 0 else mid
                    add(p, size, low, low + mid // 2)
                    folds[p, k + 1, half].start()
            else:
                add(p, size, 0, mid)
        elif k == count - 1:
            folds[p, k, h].wait_recv()
            if h == 0:
                add(p, size, mid, size)
                lasts[p].start()
            else:
                o_ref[:, mine(p)] = acc[p, 0:tok, :] + got[p, size:size + tok, :] + ident * own[:, mine(p)]
        else:
            lasts[p].wait_recv()
            o_ref[:, theirs(p)] = last[p] + ident * own[:, theirs(p)]
    for copy in gathers:
        copy.wait_send()
    for p in range(parts):
        for copy in swaps[p]:
            copy.wait_send()
        lasts[p].wait_send()
    for copy in folds.values():
        copy.wait_send()


def fused_fits(n, tok, exp_dev, capacity, width, groups):
    half = width // groups
    depth = groups * exp_dev * capacity
    block = n * tok
    firsts = len({order[0] for order in FUSED_ORDERS})
    floats = block * half + depth * half + 2 * (1 + firsts) * depth * block + block * block // 2 + 3 * tok * half
    shapes = half % (2 * PARTS * 128) == 0 and depth % 128 == 0 and block % 128 == 0 and tok % 8 == 0
    return n == 1 << FUSED_COUNT and shapes and floats * 4 <= (40 << 20)


def fused(tokens, route_ids, route_weights, expert_rows, count, groups, experts):
    n = 1 << count
    tok, top = route_ids.shape
    exp_dev, capacity, width = expert_rows.shape
    half = width // groups
    wide = half // (2 * PARTS)
    depth = groups * exp_dev * capacity
    firsts = sorted({order[0] for order in FUSED_ORDERS})
    chips = 1 + len(firsts)
    anywhere = pl.BlockSpec(memory_space=pl.ANY)
    return pl.pallas_call(
        functools.partial(fused_kernel, count, groups, experts, firsts),
        out_shape=jax.ShapeDtypeStruct((tok, half), jnp.float32),
        in_specs=[anywhere] * 4,
        out_specs=pl.BlockSpec(memory_space=pltpu.VMEM),
        scratch_shapes=[
            pltpu.VMEM((top, tok), jnp.int32),
            pltpu.VMEM((top, tok), jnp.float32),
            pltpu.VMEM((n, top, tok), jnp.int32),
            pltpu.VMEM((n, top, tok), jnp.float32),
            pltpu.VMEM((tok, half), jnp.float32),
            pltpu.VMEM((PARTS, 2 * groups, exp_dev, capacity, wide), jnp.float32),
            pltpu.VMEM((n * tok, n * tok), jnp.bfloat16),
            pltpu.VMEM((chips, depth, n * tok), jnp.float32),
            pltpu.VMEM((chips, n * tok, depth), jnp.float32),
            pltpu.VMEM((PARTS, n * tok, wide), jnp.float32),
            pltpu.VMEM((PARTS, n * tok, wide), jnp.float32),
            pltpu.VMEM((PARTS, tok, wide), jnp.float32),
            pltpu.SemaphoreType.DMA((3,)),
            pltpu.SemaphoreType.DMA((PARTS,)),
            pltpu.SemaphoreType.DMA((2, n)),
            pltpu.SemaphoreType.DMA((2, n)),
            pltpu.SemaphoreType.DMA((PARTS, 2 * groups)),
            pltpu.SemaphoreType.DMA((PARTS, 2 * groups)),
            pltpu.SemaphoreType.DMA((PARTS, count - 1, 2)),
            pltpu.SemaphoreType.DMA((PARTS, count - 1, 2)),
            pltpu.SemaphoreType.DMA((PARTS,)),
            pltpu.SemaphoreType.DMA((PARTS,)),
        ],
        compiler_params=pltpu.CompilerParams(
            collective_id=2, has_side_effects=True, vmem_limit_bytes=60 << 20
        ),
    )(tokens, route_ids.T, route_weights.T, expert_rows)


def shards(tokens, route_ids, route_weights, expert_rows):
    groups = lax.axis_size("grp")
    n = lax.axis_size("ep")
    count = n.bit_length() - 1
    group_index = lax.axis_index("grp")
    ep_index = lax.axis_index("ep")
    exp_dev, capacity, width = expert_rows.shape
    tok, top = route_ids.shape
    experts = exp_dev * groups * n
    half = width // groups
    depth = exp_dev * groups * capacity
    if fused_fits(n, tok, exp_dev, capacity, width, groups):
        return fused(tokens, route_ids, route_weights, expert_rows, count, groups, experts)

    packed = jnp.concatenate([route_ids.astype(jnp.float32), route_weights], axis=1)
    lanes = 128 if packed.size % 128 == 0 else packed.shape[1]
    everyone, *swapped = gather_small(packed.reshape(-1, lanes), expert_rows, count, groups)
    everyone = everyone.reshape((n,) + packed.shape)
    owners = [(group_index - d) % groups for d in range(groups)]
    owned = [(g * n + ep_index) * exp_dev + j for g in owners for j in range(exp_dev)]

    ids = everyone[:, :, :top].astype(jnp.int32)
    weights = everyone[:, :, top:]
    homes = jnp.stack([relative(ep_index, r) for r in range(n)])
    earlier_home = (homes[None, :] < homes[:, None]).astype(jnp.float32)
    lower = (jnp.arange(tok)[None, :] < jnp.arange(tok)[:, None]).astype(jnp.float32)
    lane = lax.broadcasted_iota(jnp.int32, (n, tok, depth), 2)
    table = jnp.zeros((n, tok, depth), jnp.float32)
    for j, expert in enumerate(owned):
        match = ids == expert
        hit = jnp.sum(match.astype(jnp.float32), axis=2)
        weight = jnp.sum(jnp.where(match, weights, 0.0), axis=2)
        before = jnp.sum(earlier_home * jnp.sum(hit, axis=1)[None, :], axis=1)
        within = jnp.sum(lower[None, :, :] * hit[:, None, :], axis=2)
        rank = (before[:, None] + within).astype(jnp.int32)
        slot = jnp.where(hit > 0, jnp.minimum(rank, capacity - 1) + j * capacity, -1)
        table = table + jnp.where(lane == slot[:, :, None], weight[:, :, None], 0.0)

    tiles = half // 128
    fits = max(1, (8 << 20) // (n * tok * 128 * 4))
    chunk = max(d for d in range(1, tiles + 1) if tiles % d == 0 and d <= fits)
    parts = max(d for d in range(1, chunk + 1) if chunk % d == 0 and d <= len(ORDERS))
    sums = [
        scatter_sum(table, expert_rows, swapped, count, parts, a * 128, chunk * 128)
        for a in range(0, tiles, chunk)
    ]
    total = sums[0] if len(sums) == 1 else jnp.concatenate(sums, axis=1)
    ident = jnp.sum(jnp.where(route_ids >= experts, route_weights, 0.0), axis=1)
    own_half = lax.dynamic_slice_in_dim(tokens, group_index * half, half, 1)
    return total + ident[:, None] * own_half


def solution(mesh):
    placed = (P("ep", None), P("ep", None), P("ep", None), P(("grp", "ep"), None, None))
    return jax.shard_map(
        shards, mesh=mesh, in_specs=placed, out_specs=P("ep", "grp"), check_vma=False
    )
```

```python
import functools

import jax
import jax.numpy as jnp
from jax import lax
from jax.experimental import pallas as pl
from jax.experimental.pallas import tpu as pltpu
from jax.sharding import PartitionSpec as P

MESH = pl.DeviceIdType.MESH
ORDERS = ((2, 0, 1, 3), (0, 2, 1, 3), (1, 3, 0, 2), (1, 3, 0, 2), (2, 0, 1, 3), (0, 1, 2, 3))


def relative(index, r):
    out, b = index, 0
    while r >> b:
        if (r >> b) & 1:
            out = out + (1 << b) * (1 - 2 * ((index // (1 << b)) % 2))
        b += 1
    return out


def fold_orders(count, parts):
    return [
        [b for b in ORDERS[p % len(ORDERS)] if b < count] + list(range(len(ORDERS[0]), count))
        for p in range(parts)
    ]


def arrival_order(orders, count):
    parts = len(orders)
    ready = [((p + 1) * 0.5, p, 0) for p in range(parts)]
    free = [0.0] * (count + 1)
    events = []
    while ready:
        start, p, s = min(ready)
        ready.remove((start, p, s))
        bit = orders[p][s]
        units = (1 << (count - 1 - s)) * 8.4 / parts
        end = max(start, free[bit]) + (2 * units if bit > 2 else units)
        free[bit] = end
        if bit > 2:
            free[2] = max(start, free[2]) + units
            end = max(end, free[2])
        events.append((end, p, s))
        if s < count - 1:
            ready.append((end + 2.5, p, s + 1))
    return [(p, s) for _, p, s in sorted(events)]


def gather_kernel(count, groups, x_ref, e_ref, o_ref, *rest):
    swapped = rest[:groups - 1]
    send_sem, recv_sem, swap_send, swap_recv = rest[groups - 1:]
    n = 1 << count
    me, grp = lax.axis_index("ep"), lax.axis_index("grp")
    half = e_ref.shape[2] // groups
    peers = [relative(me, r) for r in range(n)]
    barrier = pltpu.get_barrier_semaphore()
    others = [lax.rem(grp + d, groups) for d in range(1, groups)]
    for g in others:
        pl.semaphore_signal(barrier, inc=1, device_id={"grp": g}, device_id_type=MESH)
    for r in range(1, n):
        pl.semaphore_signal(barrier, inc=1, device_id={"ep": peers[r]}, device_id_type=MESH)
    pl.semaphore_wait(barrier, n - 1 + groups - 1)
    copies = []
    for r in range(n - 1, 0, -1):
        copies.append(pltpu.make_async_remote_copy(
            src_ref=x_ref,
            dst_ref=o_ref.at[r],
            send_sem=send_sem.at[r],
            recv_sem=recv_sem.at[r],
            device_id={"ep": peers[r]},
            device_id_type=MESH,
        ))
    for d, g in enumerate(others):
        copies.append(pltpu.make_async_remote_copy(
            src_ref=e_ref.at[:, :, pl.ds(pl.multiple_of(g * half, 128), half)],
            dst_ref=swapped[d],
            send_sem=swap_send.at[d],
            recv_sem=swap_recv.at[d],
            device_id={"grp": g},
            device_id_type=MESH,
        ))
    for copy in copies:
        copy.start()
    o_ref[0] = x_ref[...]
    for copy in copies:
        copy.wait()


def gather_small(x, expert_rows, count, groups):
    n = 1 << count
    exp_dev, capacity, width = expert_rows.shape
    swap = jax.ShapeDtypeStruct((exp_dev, capacity, width // groups), expert_rows.dtype)
    vmem, anywhere = pl.BlockSpec(memory_space=pltpu.VMEM), pl.BlockSpec(memory_space=pl.ANY)
    return pl.pallas_call(
        functools.partial(gather_kernel, count, groups),
        out_shape=[jax.ShapeDtypeStruct((n,) + x.shape, x.dtype)] + [swap] * (groups - 1),
        in_specs=[vmem, anywhere],
        out_specs=[vmem] + [anywhere] * (groups - 1),
        scratch_shapes=[
            pltpu.SemaphoreType.DMA((n,)),
            pltpu.SemaphoreType.DMA((n,)),
            pltpu.SemaphoreType.DMA((groups - 1,)),
            pltpu.SemaphoreType.DMA((groups - 1,)),
        ],
        compiler_params=pltpu.CompilerParams(collective_id=0, has_side_effects=True),
    )(x, expert_rows)


def scatter_kernel(count, parts, groups, column, c_ref, e_ref, *rest):
    swapped = rest[:groups - 1]
    o_ref, rows, acc, got, load_sem, send_sem, recv_sem = rest[groups - 1:]
    n = 1 << count
    tok = c_ref.shape[1]
    exp_dev, capacity, width = e_ref.shape
    half_width = width // groups
    wide = acc.shape[2]
    me, grp = lax.axis_index("ep"), lax.axis_index("grp")

    def loads(p):
        out = []
        start = column + p * wide
        for i in range(groups * exp_dev):
            g, e = i // exp_dev, i % exp_dev
            if g == 0:
                src = e_ref.at[e, :, pl.ds(pl.multiple_of(grp * half_width + start, 128), wide)]
            else:
                src = swapped[g - 1].at[e, :, pl.ds(start, wide)]
            dst = rows.at[p, pl.ds(i * capacity, capacity)]
            out.append(pltpu.make_async_copy(src, dst, load_sem.at[p, i]))
        return out

    loading = [loads(p) for p in range(parts)]
    for p in range(parts):
        for copy in loading[p]:
            copy.start()

    peers = [relative(me, 1 << b) for b in range(count)]
    barrier = pltpu.get_barrier_semaphore()
    for b in range(count):
        pl.semaphore_signal(barrier, inc=1, device_id={"ep": peers[b]}, device_id_type=MESH)
    orders = fold_orders(count, parts)

    def place(p, q):
        return sum(((q >> (count - 1 - s)) & 1) << orders[p][s] for s in range(count))

    def multiply(p, low, high):
        weights = jnp.concatenate([c_ref[place(p, q)] for q in range(low, high)], axis=0)
        acc[p, low * tok:high * tok, :] = jnp.dot(
            weights,
            rows[p],
            preferred_element_type=jnp.float32,
            precision=lax.Precision.HIGHEST,
        )

    def transfer(p, s):
        half = (n >> (s + 1)) * tok
        return pltpu.make_async_remote_copy(
            src_ref=acc.at[p, pl.ds(half, half)],
            dst_ref=got.at[p, pl.ds(half, half)],
            send_sem=send_sem.at[p, s],
            recv_sem=recv_sem.at[p, s],
            device_id={"ep": peers[orders[p][s]]},
            device_id_type=MESH,
        )

    copies = [[transfer(p, s) for s in range(count)] for p in range(parts)]
    for p in range(parts):
        for copy in loading[p]:
            copy.wait()
        multiply(p, n // 2, n)
        if p == 0:
            pl.semaphore_wait(barrier, count)
        copies[p][0].start()
    for p in range(parts):
        multiply(p, 0, n // 2)
    for p, s in arrival_order(orders, count):
        half = (n >> (s + 1)) * tok
        copies[p][s].wait_recv()
        if s < count - 1:
            mid = half // 2
            acc[p, mid:half, :] += got[p, half + mid:2 * half, :]
            copies[p][s + 1].start()
            acc[p, 0:mid, :] += got[p, half:half + mid, :]
        else:
            o_ref[:, p * wide:(p + 1) * wide] = acc[p, 0:tok, :] + got[p, tok:2 * tok, :]
    for p in range(parts):
        for s in range(count):
            copies[p][s].wait_send()


def scatter_sum(c, expert_rows, swapped, count, parts, column, span):
    n, tok, depth = c.shape
    groups = len(swapped) + 1
    wide = span // parts
    vmem, anywhere = pl.BlockSpec(memory_space=pltpu.VMEM), pl.BlockSpec(memory_space=pl.ANY)
    return pl.pallas_call(
        functools.partial(scatter_kernel, count, parts, groups, column),
        out_shape=jax.ShapeDtypeStruct((tok, span), jnp.float32),
        in_specs=[vmem, anywhere] + [anywhere] * (groups - 1),
        out_specs=vmem,
        scratch_shapes=[
            pltpu.VMEM((parts, depth, wide), jnp.float32),
            pltpu.VMEM((parts, n * tok, wide), jnp.float32),
            pltpu.VMEM((parts, n * tok, wide), jnp.float32),
            pltpu.SemaphoreType.DMA((parts, groups * expert_rows.shape[0])),
            pltpu.SemaphoreType.DMA((parts, count)),
            pltpu.SemaphoreType.DMA((parts, count)),
        ],
        compiler_params=pltpu.CompilerParams(
            collective_id=1, has_side_effects=True, vmem_limit_bytes=60 << 20
        ),
    )(c, expert_rows, *swapped)


PARTS = 6
FUSED_COUNT = 4
EARLY = 3
FUSED_ORDERS = (
        (2, 1, 3, 0), (0, 1, 2, 3), (1, 2, 0, 3), (2, 0, 1, 3), (0, 1, 2, 3), (0, 1, 2, 3),
)
FUSED_SEQUENCE = (
        (0, 0, 0), (1, 0, 0), (2, 0, 0), (0, 1, 0), (0, 1, 1), (3, 0, 0), (4, 0, 0), (1, 1, 0), (2, 1, 0), (1, 1, 1),
        (0, 2, 0), (2, 1, 1), (4, 1, 0), (5, 0, 0), (0, 2, 1), (1, 2, 0), (3, 1, 0), (1, 2, 1), (4, 1, 1), (4, 2, 0),
        (3, 1, 1), (5, 1, 0), (4, 2, 1), (1, 3, 0), (2, 2, 0), (5, 1, 1), (0, 3, 0), (1, 3, 1), (0, 3, 1), (2, 2, 1),
        (3, 2, 0), (1, 4, 0), (4, 3, 0), (3, 2, 1), (4, 3, 1), (5, 2, 0), (4, 4, 0), (5, 2, 1), (0, 4, 0), (2, 3, 0),
        (2, 3, 1), (3, 3, 0), (2, 4, 0), (3, 3, 1), (5, 3, 0), (5, 3, 1), (3, 4, 0), (5, 4, 0),
)


def packed_shape(top, tok):
    return (8, -(-(2 * top // 8) * tok // 128) * 128)


def pack(both, shape):
    blocks = [both[i:i + 8] for i in range(0, both.shape[0], 8)]
    room = shape[1] - len(blocks) * both.shape[1]
    if room:
        blocks.append(jnp.zeros((8, room), both.dtype))
    return jnp.concatenate(blocks, axis=1)


def unpack(tile, height, tok):
    return jnp.concatenate([tile[:, i * tok:(i + 1) * tok] for i in range(height // 8)], axis=0)


def fused_kernel(count, groups, experts, firsts, t_ref, i_ref, w_ref, e_ref, o_ref, ids_own, w_own, packed,
                 own, rows, lower, flat, table, acc, got, last, small_sem, load_sem, present, gather_send, gather_recv,
                 swap_send, swap_recv, fold_send, fold_recv, last_send, last_recv):
    n = 1 << count
    top, tok = i_ref.shape
    exp_dev, capacity, width = e_ref.shape
    half_width = width // groups
    wide = acc.shape[2]
    parts = acc.shape[0]
    depth = groups * exp_dev * capacity
    orders = FUSED_ORDERS
    me, grp = lax.axis_index("ep"), lax.axis_index("grp")
    peers = [relative(me, r) for r in range(n)]
    others = [lax.rem(grp + d, groups) for d in range(1, groups)]
    sides = [lax.rem(me // (1 << orders[p][0]), 2) for p in range(parts)]

    def mine(p):
        return pl.ds(pl.multiple_of(2 * p * wide + sides[p] * wide, 128), wide)

    def theirs(p):
        return pl.ds(pl.multiple_of(2 * p * wide + (1 - sides[p]) * wide, 128), wide)

    def source(g, p, side):
        return e_ref.at[:, :, pl.ds(pl.multiple_of(g * half_width + 2 * p * wide + side * wide, 128), wide)]

    smalls = [
        pltpu.make_async_copy(i_ref, ids_own, small_sem.at[0]),
        pltpu.make_async_copy(w_ref, w_own, small_sem.at[1]),
        pltpu.make_async_copy(
            t_ref.at[:, pl.ds(pl.multiple_of(grp * half_width, 128), half_width)], own, small_sem.at[2]
        ),
    ]
    for copy in smalls:
        copy.start()
    barrier = pltpu.get_barrier_semaphore()
    for b in range(count):
        pl.semaphore_signal(barrier, inc=1, device_id={"ep": peers[1 << b]}, device_id_type=MESH)
    for g in others:
        for b in firsts:
            pl.semaphore_signal(barrier, inc=1, device_id={"grp": g, "ep": peers[1 << b]}, device_id_type=MESH)
        pl.semaphore_signal(barrier, inc=1, device_id={"grp": g}, device_id_type=MESH)

    loads = [pltpu.make_async_copy(source(grp, p, sides[p]), rows.at[p, 0], load_sem.at[p]) for p in range(parts)]
    for copy in loads:
        copy.start()

    block = n * tok
    across = jnp.concatenate(
        [lax.broadcasted_iota(jnp.int32, (1, tok), 1) + peers[r] * tok for r in range(n)], axis=1
    )
    down = jnp.concatenate(
        [lax.broadcasted_iota(jnp.int32, (tok, 1), 0) + peers[r] * tok for r in range(n)], axis=0
    )
    lower[...] = jnp.where(down < across, 1.0, 0.0).astype(lower.dtype)

    smalls[0].wait()
    smalls[1].wait()
    both = jnp.concatenate([ids_own[...].astype(jnp.float32), w_own[...]], axis=0)
    packed[0] = pack(both, packed.shape[1:])
    pl.semaphore_wait(barrier, count + (groups - 1) * (1 + len(firsts)))
    def swap(p, slot, e):
        c, d = slot // groups, slot % groups
        to = {}
        if c:
            to["ep"] = peers[1 << orders[p][0]]
        if d:
            to["grp"] = others[d - 1]
        return pltpu.make_async_remote_copy(
            src_ref=source(lax.rem(grp + d, groups), p, 1 - sides[p] if c else sides[p]).at[e],
            dst_ref=rows.at[p, slot, e],
            send_sem=swap_send.at[p, slot, e],
            recv_sem=swap_recv.at[p, slot, e],
            device_id=to,
            device_id_type=MESH,
        )

    swaps = [
        [swap(p, slot, e) for slot in range(2 * groups - 1, 0, -1) for e in range(exp_dev)] for p in range(parts)
    ]
    far = groups * exp_dev
    heads = [min(p for p in range(parts) if orders[p][0] == b) for b in firsts]
    early = [(p, i) for i in range(min(far, EARLY)) for p in heads]
    later = [(p, i) for p in range(parts) for i in range(len(swaps[p])) if (p, i) not in early]
    for p, i in early:
        swaps[p][i].start()
    for p in range(parts):
        for i in range(far, len(swaps[p])):
            swaps[p][i].start()
    for b in range(count - 2, -1, -1):
        pl.semaphore_signal(present.at[b], inc=1, device_id={"ep": peers[1 << b]}, device_id_type=MESH)
        pl.semaphore_wait(present.at[b], 1)
    spread = []
    for r in range(n - 1, 0, -1):
        spread.append(pltpu.make_async_remote_copy(
            src_ref=packed.at[0],
            dst_ref=packed.at[r],
            send_sem=gather_send.at[r],
            recv_sem=gather_recv.at[r],
            device_id={"ep": peers[r]},
            device_id_type=MESH,
        ))
        spread[-1].start()
    for p, i in later:
        if i < far:
            swaps[p][i].start()

    chosen = ids_own[...]
    ident_row = jnp.sum(jnp.where(chosen >= experts, w_own[...], 0.0), axis=0, keepdims=True)
    eye = lax.broadcasted_iota(jnp.int32, (tok, tok), 0) == lax.broadcasted_iota(jnp.int32, (tok, tok), 1)
    ident = jnp.sum(jnp.where(eye, ident_row, 0.0), axis=1, keepdims=True)
    smalls[2].wait()

    for copy in spread:
        copy.wait_recv()
    both = jnp.concatenate([both] + [unpack(packed[r], 2 * top, tok) for r in range(1, n)], axis=1)
    ids = both[:top].astype(jnp.int32)
    weights = both[top:]
    chips = [me] + [peers[1 << b] for b in firsts]
    hits, picked = [], []
    for chip in chips:
        for d in range(groups):
            for e in range(exp_dev):
                expert = (lax.rem(grp + groups - d, groups) * n + chip) * exp_dev + e
                match = ids == expert
                hits.append(jnp.sum(jnp.where(match, 1.0, 0.0), axis=0, keepdims=True))
                picked.append(jnp.sum(jnp.where(match, weights, 0.0), axis=0, keepdims=True))
    hit = jnp.concatenate(hits, axis=0)
    rank = jnp.dot(hit.astype(lower.dtype), lower[...], preferred_element_type=jnp.float32)
    slots = jnp.where(hit > 0.0, rank, -1.0)
    level = lax.broadcasted_iota(jnp.int32, (capacity, block), 0).astype(jnp.float32)
    each = groups * exp_dev
    for c in range(len(chips)):
        for j in range(each):
            i = c * each + j
            flat[c, j * capacity:(j + 1) * capacity, :] = jnp.where(level == slots[i:i + 1, :], picked[i], 0.0)
        table[c] = jnp.transpose(flat[c])

    def place(p, q):
        out = (q % 2) << orders[p][0]
        return out + sum(((q >> (count - k)) & 1) << orders[p][k] for k in range(1, count))

    def multiply(p, low, high):
        c = 1 + firsts.index(orders[p][0])
        spots = [pl.ds(place(p, q) * tok, tok) for q in range(low, high)]
        left = jnp.concatenate(
            [jnp.concatenate([table[x, spot, :] for spot in spots], axis=0) for x in (0, c)], axis=1
        )
        acc[p, low * tok:high * tok, :] = jnp.dot(
            left,
            rows[p].reshape(2 * depth, wide),
            preferred_element_type=jnp.float32,
            precision=lax.Precision.HIGHEST,
        )

    def fold(p, k, h):
        size = (n >> k) * tok
        mid = size // 2
        where = pl.ds(size + mid if h == 0 else size, mid)
        return pltpu.make_async_remote_copy(
            src_ref=acc.at[p, where],
            dst_ref=got.at[p, where],
            send_sem=fold_send.at[p, k - 1, h],
            recv_sem=fold_recv.at[p, k - 1, h],
            device_id={"ep": peers[1 << orders[p][k]]},
            device_id_type=MESH,
        )

    folds = {(p, k, h): fold(p, k, h) for p in range(parts) for k in range(1, count) for h in range(2)}
    lasts = [
        pltpu.make_async_remote_copy(
            src_ref=acc.at[p, pl.ds(tok, tok)],
            dst_ref=last.at[p],
            send_sem=last_send.at[p],
            recv_sem=last_recv.at[p],
            device_id={"ep": peers[1 << orders[p][0]]},
            device_id_type=MESH,
        )
        for p in range(parts)
    ]

    def add(p, size, low, high):
        acc[p, low:high, :] += got[p, size + low:size + high, :]

    for p, k, h in FUSED_SEQUENCE:
        size = (n >> k) * tok
        mid = size // 2
        if k == 0:
            loads[p].wait()
            for copy in swaps[p]:
                copy.wait_recv()
            multiply(p, n // 2, n)
            folds[p, 1, 0].start()
            folds[p, 1, 1].start()
            multiply(p, 0, n // 2)
        elif k < count - 1:
            folds[p, k, h].wait_recv()
            if h == 0:
                for half in range(2):
                    low = mid + mid // 2 if half == 0 else mid
                    add(p, size, low, low + mid // 2)
                    folds[p, k + 1, half].start()
            else:
                add(p, size, 0, mid)
        elif k == count - 1:
            folds[p, k, h].wait_recv()
            if h == 0:
                add(p, size, mid, size)
                lasts[p].start()
            else:
                o_ref[:, mine(p)] = acc[p, 0:tok, :] + got[p, size:size + tok, :] + ident * own[:, mine(p)]
        else:
            lasts[p].wait_recv()
            o_ref[:, theirs(p)] = last[p] + ident * own[:, theirs(p)]
    for copy in spread:
        copy.wait_send()
    for p in range(parts):
        for copy in swaps[p]:
            copy.wait_send()
        lasts[p].wait_send()
    for copy in folds.values():
        copy.wait_send()


def fused_fits(n, tok, top, exp_dev, capacity, width, groups):
    half = width // groups
    depth = groups * exp_dev * capacity
    block = n * tok
    firsts = len({order[0] for order in FUSED_ORDERS})
    floats = block * half + depth * half + 2 * (1 + firsts) * depth * block + block * block // 2 + 3 * tok * half
    shapes = 2 * top % 8 == 0 and half % (2 * PARTS * 128) == 0 and depth % 128 == 0 and block % 128 == 0 and tok % 8 == 0
    return n == 1 << FUSED_COUNT and shapes and floats * 4 <= (40 << 20)


def fused(tokens, route_ids, route_weights, expert_rows, count, groups, experts):
    n = 1 << count
    tok, top = route_ids.shape
    exp_dev, capacity, width = expert_rows.shape
    half = width // groups
    wide = half // (2 * PARTS)
    depth = groups * exp_dev * capacity
    firsts = sorted({order[0] for order in FUSED_ORDERS})
    chips = 1 + len(firsts)
    anywhere = pl.BlockSpec(memory_space=pl.ANY)
    return pl.pallas_call(
        functools.partial(fused_kernel, count, groups, experts, firsts),
        out_shape=jax.ShapeDtypeStruct((tok, half), jnp.float32),
        in_specs=[anywhere] * 4,
        out_specs=pl.BlockSpec(memory_space=pltpu.VMEM),
        scratch_shapes=[
            pltpu.VMEM((top, tok), jnp.int32),
            pltpu.VMEM((top, tok), jnp.float32),
            pltpu.VMEM((n,) + packed_shape(top, tok), jnp.float32),
            pltpu.VMEM((tok, half), jnp.float32),
            pltpu.VMEM((PARTS, 2 * groups, exp_dev, capacity, wide), jnp.float32),
            pltpu.VMEM((n * tok, n * tok), jnp.bfloat16),
            pltpu.VMEM((chips, depth, n * tok), jnp.float32),
            pltpu.VMEM((chips, n * tok, depth), jnp.float32),
            pltpu.VMEM((PARTS, n * tok, wide), jnp.float32),
            pltpu.VMEM((PARTS, n * tok, wide), jnp.float32),
            pltpu.VMEM((PARTS, tok, wide), jnp.float32),
            pltpu.SemaphoreType.DMA((3,)),
            pltpu.SemaphoreType.DMA((PARTS,)),
            pltpu.SemaphoreType.REGULAR((count - 1,)),
            pltpu.SemaphoreType.DMA((n,)),
            pltpu.SemaphoreType.DMA((n,)),
            pltpu.SemaphoreType.DMA((PARTS, 2 * groups, exp_dev)),
            pltpu.SemaphoreType.DMA((PARTS, 2 * groups, exp_dev)),
            pltpu.SemaphoreType.DMA((PARTS, count - 1, 2)),
            pltpu.SemaphoreType.DMA((PARTS, count - 1, 2)),
            pltpu.SemaphoreType.DMA((PARTS,)),
            pltpu.SemaphoreType.DMA((PARTS,)),
        ],
        compiler_params=pltpu.CompilerParams(
            collective_id=2, has_side_effects=True, vmem_limit_bytes=53 << 20
        ),
    )(tokens, route_ids.T, route_weights.T, expert_rows)


def shards(tokens, route_ids, route_weights, expert_rows):
    groups = lax.axis_size("grp")
    n = lax.axis_size("ep")
    count = n.bit_length() - 1
    group_index = lax.axis_index("grp")
    ep_index = lax.axis_index("ep")
    exp_dev, capacity, width = expert_rows.shape
    tok, top = route_ids.shape
    experts = exp_dev * groups * n
    half = width // groups
    depth = exp_dev * groups * capacity
    if fused_fits(n, tok, top, exp_dev, capacity, width, groups):
        return fused(tokens, route_ids, route_weights, expert_rows, count, groups, experts)

    packed = jnp.concatenate([route_ids.astype(jnp.float32), route_weights], axis=1)
    lanes = 128 if packed.size % 128 == 0 else packed.shape[1]
    everyone, *swapped = gather_small(packed.reshape(-1, lanes), expert_rows, count, groups)
    everyone = everyone.reshape((n,) + packed.shape)
    owners = [(group_index - d) % groups for d in range(groups)]
    owned = [(g * n + ep_index) * exp_dev + j for g in owners for j in range(exp_dev)]

    ids = everyone[:, :, :top].astype(jnp.int32)
    weights = everyone[:, :, top:]
    homes = jnp.stack([relative(ep_index, r) for r in range(n)])
    earlier_home = (homes[None, :] < homes[:, None]).astype(jnp.float32)
    lower = (jnp.arange(tok)[None, :] < jnp.arange(tok)[:, None]).astype(jnp.float32)
    lane = lax.broadcasted_iota(jnp.int32, (n, tok, depth), 2)
    table = jnp.zeros((n, tok, depth), jnp.float32)
    for j, expert in enumerate(owned):
        match = ids == expert
        hit = jnp.sum(match.astype(jnp.float32), axis=2)
        weight = jnp.sum(jnp.where(match, weights, 0.0), axis=2)
        before = jnp.sum(earlier_home * jnp.sum(hit, axis=1)[None, :], axis=1)
        within = jnp.sum(lower[None, :, :] * hit[:, None, :], axis=2)
        rank = (before[:, None] + within).astype(jnp.int32)
        slot = jnp.where(hit > 0, jnp.minimum(rank, capacity - 1) + j * capacity, -1)
        table = table + jnp.where(lane == slot[:, :, None], weight[:, :, None], 0.0)

    tiles = half // 128
    fits = max(1, (8 << 20) // (n * tok * 128 * 4))
    chunk = max(d for d in range(1, tiles + 1) if tiles % d == 0 and d <= fits)
    parts = max(d for d in range(1, chunk + 1) if chunk % d == 0 and d <= len(ORDERS))
    sums = [
        scatter_sum(table, expert_rows, swapped, count, parts, a * 128, chunk * 128)
        for a in range(0, tiles, chunk)
    ]
    total = sums[0] if len(sums) == 1 else jnp.concatenate(sums, axis=1)
    ident = jnp.sum(jnp.where(route_ids >= experts, route_weights, 0.0), axis=1)
    own_half = lax.dynamic_slice_in_dim(tokens, group_index * half, half, 1)
    return total + ident[:, None] * own_half


def solution(mesh):
    placed = (P("ep", None), P("ep", None), P("ep", None), P(("grp", "ep"), None, None))
    return jax.shard_map(
        shards, mesh=mesh, in_specs=placed, out_specs=P("ep", "grp"), check_vma=False
    )
```

```python
import functools

import jax
import jax.numpy as jnp
from jax import lax
from jax.experimental import pallas as pl
from jax.experimental.pallas import tpu as pltpu
from jax.sharding import PartitionSpec as P

MESH = pl.DeviceIdType.MESH
ORDERS = ((2, 0, 1, 3), (0, 2, 1, 3), (1, 3, 0, 2), (1, 3, 0, 2), (2, 0, 1, 3), (0, 1, 2, 3))


def relative(index, r):
    out, b = index, 0
    while r >> b:
        if (r >> b) & 1:
            out = out + (1 << b) * (1 - 2 * ((index // (1 << b)) % 2))
        b += 1
    return out


def fold_orders(count, parts):
    return [
        [b for b in ORDERS[p % len(ORDERS)] if b < count] + list(range(len(ORDERS[0]), count))
        for p in range(parts)
    ]


def arrival_order(orders, count):
    parts = len(orders)
    ready = [((p + 1) * 0.5, p, 0) for p in range(parts)]
    free = [0.0] * (count + 1)
    events = []
    while ready:
        start, p, s = min(ready)
        ready.remove((start, p, s))
        bit = orders[p][s]
        units = (1 << (count - 1 - s)) * 8.4 / parts
        end = max(start, free[bit]) + (2 * units if bit > 2 else units)
        free[bit] = end
        if bit > 2:
            free[2] = max(start, free[2]) + units
            end = max(end, free[2])
        events.append((end, p, s))
        if s < count - 1:
            ready.append((end + 2.5, p, s + 1))
    return [(p, s) for _, p, s in sorted(events)]


def gather_kernel(count, groups, x_ref, e_ref, o_ref, *rest):
    swapped = rest[:groups - 1]
    send_sem, recv_sem, swap_send, swap_recv = rest[groups - 1:]
    n = 1 << count
    me, grp = lax.axis_index("ep"), lax.axis_index("grp")
    half = e_ref.shape[2] // groups
    peers = [relative(me, r) for r in range(n)]
    barrier = pltpu.get_barrier_semaphore()
    others = [lax.rem(grp + d, groups) for d in range(1, groups)]
    for g in others:
        pl.semaphore_signal(barrier, inc=1, device_id={"grp": g}, device_id_type=MESH)
    for r in range(1, n):
        pl.semaphore_signal(barrier, inc=1, device_id={"ep": peers[r]}, device_id_type=MESH)
    pl.semaphore_wait(barrier, n - 1 + groups - 1)
    copies = []
    for r in range(n - 1, 0, -1):
        copies.append(pltpu.make_async_remote_copy(
            src_ref=x_ref,
            dst_ref=o_ref.at[r],
            send_sem=send_sem.at[r],
            recv_sem=recv_sem.at[r],
            device_id={"ep": peers[r]},
            device_id_type=MESH,
        ))
    for d, g in enumerate(others):
        copies.append(pltpu.make_async_remote_copy(
            src_ref=e_ref.at[:, :, pl.ds(pl.multiple_of(g * half, 128), half)],
            dst_ref=swapped[d],
            send_sem=swap_send.at[d],
            recv_sem=swap_recv.at[d],
            device_id={"grp": g},
            device_id_type=MESH,
        ))
    for copy in copies:
        copy.start()
    o_ref[0] = x_ref[...]
    for copy in copies:
        copy.wait()


def gather_small(x, expert_rows, count, groups):
    n = 1 << count
    exp_dev, capacity, width = expert_rows.shape
    swap = jax.ShapeDtypeStruct((exp_dev, capacity, width // groups), expert_rows.dtype)
    vmem, anywhere = pl.BlockSpec(memory_space=pltpu.VMEM), pl.BlockSpec(memory_space=pl.ANY)
    return pl.pallas_call(
        functools.partial(gather_kernel, count, groups),
        out_shape=[jax.ShapeDtypeStruct((n,) + x.shape, x.dtype)] + [swap] * (groups - 1),
        in_specs=[vmem, anywhere],
        out_specs=[vmem] + [anywhere] * (groups - 1),
        scratch_shapes=[
            pltpu.SemaphoreType.DMA((n,)),
            pltpu.SemaphoreType.DMA((n,)),
            pltpu.SemaphoreType.DMA((groups - 1,)),
            pltpu.SemaphoreType.DMA((groups - 1,)),
        ],
        compiler_params=pltpu.CompilerParams(collective_id=0, has_side_effects=True),
    )(x, expert_rows)


def scatter_kernel(count, parts, groups, column, c_ref, e_ref, *rest):
    swapped = rest[:groups - 1]
    o_ref, rows, acc, got, load_sem, send_sem, recv_sem = rest[groups - 1:]
    n = 1 << count
    tok = c_ref.shape[1]
    exp_dev, capacity, width = e_ref.shape
    half_width = width // groups
    wide = acc.shape[2]
    me, grp = lax.axis_index("ep"), lax.axis_index("grp")

    def loads(p):
        out = []
        start = column + p * wide
        for i in range(groups * exp_dev):
            g, e = i // exp_dev, i % exp_dev
            if g == 0:
                src = e_ref.at[e, :, pl.ds(pl.multiple_of(grp * half_width + start, 128), wide)]
            else:
                src = swapped[g - 1].at[e, :, pl.ds(start, wide)]
            dst = rows.at[p, pl.ds(i * capacity, capacity)]
            out.append(pltpu.make_async_copy(src, dst, load_sem.at[p, i]))
        return out

    loading = [loads(p) for p in range(parts)]
    for p in range(parts):
        for copy in loading[p]:
            copy.start()

    peers = [relative(me, 1 << b) for b in range(count)]
    barrier = pltpu.get_barrier_semaphore()
    for b in range(count):
        pl.semaphore_signal(barrier, inc=1, device_id={"ep": peers[b]}, device_id_type=MESH)
    orders = fold_orders(count, parts)

    def place(p, q):
        return sum(((q >> (count - 1 - s)) & 1) << orders[p][s] for s in range(count))

    def multiply(p, low, high):
        weights = jnp.concatenate([c_ref[place(p, q)] for q in range(low, high)], axis=0)
        acc[p, low * tok:high * tok, :] = jnp.dot(
            weights,
            rows[p],
            preferred_element_type=jnp.float32,
            precision=lax.Precision.HIGHEST,
        )

    def transfer(p, s):
        half = (n >> (s + 1)) * tok
        return pltpu.make_async_remote_copy(
            src_ref=acc.at[p, pl.ds(half, half)],
            dst_ref=got.at[p, pl.ds(half, half)],
            send_sem=send_sem.at[p, s],
            recv_sem=recv_sem.at[p, s],
            device_id={"ep": peers[orders[p][s]]},
            device_id_type=MESH,
        )

    copies = [[transfer(p, s) for s in range(count)] for p in range(parts)]
    for p in range(parts):
        for copy in loading[p]:
            copy.wait()
        multiply(p, n // 2, n)
        if p == 0:
            pl.semaphore_wait(barrier, count)
        copies[p][0].start()
    for p in range(parts):
        multiply(p, 0, n // 2)
    for p, s in arrival_order(orders, count):
        half = (n >> (s + 1)) * tok
        copies[p][s].wait_recv()
        if s < count - 1:
            mid = half // 2
            acc[p, mid:half, :] += got[p, half + mid:2 * half, :]
            copies[p][s + 1].start()
            acc[p, 0:mid, :] += got[p, half:half + mid, :]
        else:
            o_ref[:, p * wide:(p + 1) * wide] = acc[p, 0:tok, :] + got[p, tok:2 * tok, :]
    for p in range(parts):
        for s in range(count):
            copies[p][s].wait_send()


def scatter_sum(c, expert_rows, swapped, count, parts, column, span):
    n, tok, depth = c.shape
    groups = len(swapped) + 1
    wide = span // parts
    vmem, anywhere = pl.BlockSpec(memory_space=pltpu.VMEM), pl.BlockSpec(memory_space=pl.ANY)
    return pl.pallas_call(
        functools.partial(scatter_kernel, count, parts, groups, column),
        out_shape=jax.ShapeDtypeStruct((tok, span), jnp.float32),
        in_specs=[vmem, anywhere] + [anywhere] * (groups - 1),
        out_specs=vmem,
        scratch_shapes=[
            pltpu.VMEM((parts, depth, wide), jnp.float32),
            pltpu.VMEM((parts, n * tok, wide), jnp.float32),
            pltpu.VMEM((parts, n * tok, wide), jnp.float32),
            pltpu.SemaphoreType.DMA((parts, groups * expert_rows.shape[0])),
            pltpu.SemaphoreType.DMA((parts, count)),
            pltpu.SemaphoreType.DMA((parts, count)),
        ],
        compiler_params=pltpu.CompilerParams(
            collective_id=1, has_side_effects=True, vmem_limit_bytes=60 << 20
        ),
    )(c, expert_rows, *swapped)


WIDTHS = (2, 2, 2, 2, 2, 2)
PARTS = len(WIDTHS)
FUSED_COUNT = 4
EARLY = 4
FUSED_ORDERS = (
        (2, 0, 3, 1), (1, 0, 2, 3), (1, 0, 2, 3), (0, 2, 1, 3), (1, 0, 2, 3), (2, 1, 0, 3),
)
FUSED_SEQUENCE = (
        (0, 0, 0), (1, 0, 0), (3, 0, 0), (0, 1, 0), (0, 1, 1), (5, 0, 0), (2, 0, 0), (1, 1, 0), (3, 1, 0), (1, 1, 1),
        (0, 2, 0), (3, 1, 1), (2, 1, 0), (4, 0, 0), (0, 2, 1), (1, 2, 0), (5, 1, 0), (1, 2, 1), (2, 1, 1), (2, 2, 0),
        (5, 1, 1), (4, 1, 0), (2, 2, 1), (1, 3, 0), (3, 2, 0), (4, 1, 1), (0, 3, 0), (1, 3, 1), (0, 3, 1), (3, 2, 1),
        (5, 2, 0), (1, 4, 0), (2, 3, 0), (5, 2, 1), (2, 3, 1), (4, 2, 0), (2, 4, 0), (4, 2, 1), (0, 4, 0), (3, 3, 0),
        (3, 3, 1), (5, 3, 0), (3, 4, 0), (5, 3, 1), (4, 3, 0), (4, 3, 1), (5, 4, 0), (4, 4, 0),
)


def packed_shape(top, tok):
    return (8, -(-(2 * top // 8) * tok // 128) * 128)


def pack(both, shape):
    blocks = [both[i:i + 8] for i in range(0, both.shape[0], 8)]
    room = shape[1] - len(blocks) * both.shape[1]
    if room:
        blocks.append(jnp.zeros((8, room), both.dtype))
    return jnp.concatenate(blocks, axis=1)


def unpack(tile, height, tok):
    return jnp.concatenate([tile[:, i * tok:(i + 1) * tok] for i in range(height // 8)], axis=0)


def fused_kernel(count, groups, experts, firsts, t_ref, i_ref, w_ref, e_ref, o_ref, ids_own, w_own, packed,
                 own, lower, flat, table, small_sem, load_sem, present, gather_send, gather_recv,
                 swap_send, swap_recv, fold_send, fold_recv, last_send, last_recv, *buffers):
    n = 1 << count
    top, tok = i_ref.shape
    exp_dev, capacity, width = e_ref.shape
    half_width = width // groups
    parts = PARTS
    rows, acc, got, last = [buffers[i * parts:(i + 1) * parts] for i in range(4)]
    wide = [ref.shape[1] for ref in acc]
    first = [2 * sum(wide[:p]) for p in range(parts)]
    depth = groups * exp_dev * capacity
    orders = FUSED_ORDERS
    me, grp = lax.axis_index("ep"), lax.axis_index("grp")
    peers = [relative(me, r) for r in range(n)]
    others = [lax.rem(grp + d, groups) for d in range(1, groups)]
    sides = [lax.rem(me // (1 << orders[p][0]), 2) for p in range(parts)]

    def mine(p):
        return pl.ds(pl.multiple_of(first[p] + sides[p] * wide[p], 128), wide[p])

    def theirs(p):
        return pl.ds(pl.multiple_of(first[p] + (1 - sides[p]) * wide[p], 128), wide[p])

    def source(g, p, side):
        return e_ref.at[:, :, pl.ds(pl.multiple_of(g * half_width + first[p] + side * wide[p], 128), wide[p])]

    smalls = [
        pltpu.make_async_copy(i_ref, ids_own, small_sem.at[0]),
        pltpu.make_async_copy(w_ref, w_own, small_sem.at[1]),
        pltpu.make_async_copy(
            t_ref.at[:, pl.ds(pl.multiple_of(grp * half_width, 128), half_width)], own, small_sem.at[2]
        ),
    ]
    for copy in smalls:
        copy.start()
    barrier = pltpu.get_barrier_semaphore()
    for b in range(count):
        pl.semaphore_signal(barrier, inc=1, device_id={"ep": peers[1 << b]}, device_id_type=MESH)
    for g in others:
        for b in firsts:
            pl.semaphore_signal(barrier, inc=1, device_id={"grp": g, "ep": peers[1 << b]}, device_id_type=MESH)
        pl.semaphore_signal(barrier, inc=1, device_id={"grp": g}, device_id_type=MESH)

    loads = [pltpu.make_async_copy(source(grp, p, sides[p]), rows[p].at[0], load_sem.at[p]) for p in range(parts)]
    for copy in loads:
        copy.start()

    block = n * tok
    across = jnp.concatenate(
        [lax.broadcasted_iota(jnp.int32, (1, tok), 1) + peers[r] * tok for r in range(n)], axis=1
    )
    down = jnp.concatenate(
        [lax.broadcasted_iota(jnp.int32, (tok, 1), 0) + peers[r] * tok for r in range(n)], axis=0
    )
    lower[...] = jnp.where(down < across, 1.0, 0.0).astype(lower.dtype)

    smalls[0].wait()
    smalls[1].wait()
    both = jnp.concatenate([ids_own[...].astype(jnp.float32), w_own[...]], axis=0)
    packed[0] = pack(both, packed.shape[1:])
    pl.semaphore_wait(barrier, count + (groups - 1) * (1 + len(firsts)))
    def swap(p, slot, e):
        c, d = slot // groups, slot % groups
        to = {}
        if c:
            to["ep"] = peers[1 << orders[p][0]]
        if d:
            to["grp"] = others[d - 1]
        return pltpu.make_async_remote_copy(
            src_ref=source(lax.rem(grp + d, groups), p, 1 - sides[p] if c else sides[p]).at[e],
            dst_ref=rows[p].at[slot, e],
            send_sem=swap_send.at[p, slot, e],
            recv_sem=swap_recv.at[p, slot, e],
            device_id=to,
            device_id_type=MESH,
        )

    swaps = [
        [swap(p, slot, e) for slot in range(2 * groups - 1, 0, -1) for e in range(exp_dev)] for p in range(parts)
    ]
    far = groups * exp_dev
    queues = [[(p, i) for p in range(parts) if orders[p][0] == b for i in range(far)] for b in firsts]
    early = [
        (p, i) for queue in queues for at, (p, i) in enumerate(queue)
        if sum(wide[x] for x, _ in queue[:at]) < half_width // EARLY
    ]
    later = [(p, i) for p in range(parts) for i in range(len(swaps[p])) if (p, i) not in early]
    for p, i in early:
        swaps[p][i].start()
    for p in range(parts):
        for i in range(far, len(swaps[p])):
            swaps[p][i].start()
    for b in range(count - 2, -1, -1):
        pl.semaphore_signal(present.at[b], inc=1, device_id={"ep": peers[1 << b]}, device_id_type=MESH)
        pl.semaphore_wait(present.at[b], 1)
    spread = []
    for r in range(n - 1, 0, -1):
        spread.append(pltpu.make_async_remote_copy(
            src_ref=packed.at[0],
            dst_ref=packed.at[r],
            send_sem=gather_send.at[r],
            recv_sem=gather_recv.at[r],
            device_id={"ep": peers[r]},
            device_id_type=MESH,
        ))
        spread[-1].start()
    for p, i in later:
        if i < far:
            swaps[p][i].start()

    chosen = ids_own[...]
    ident_row = jnp.sum(jnp.where(chosen >= experts, w_own[...], 0.0), axis=0, keepdims=True)
    eye = lax.broadcasted_iota(jnp.int32, (tok, tok), 0) == lax.broadcasted_iota(jnp.int32, (tok, tok), 1)
    ident = jnp.sum(jnp.where(eye, ident_row, 0.0), axis=1, keepdims=True)
    smalls[2].wait()

    for copy in spread:
        copy.wait_recv()
    both = jnp.concatenate([both] + [unpack(packed[r], 2 * top, tok) for r in range(1, n)], axis=1)
    ids = both[:top].astype(jnp.int32)
    weights = both[top:]
    chips = [me] + [peers[1 << b] for b in firsts]
    hits, picked = [], []
    for chip in chips:
        for d in range(groups):
            for e in range(exp_dev):
                expert = (lax.rem(grp + groups - d, groups) * n + chip) * exp_dev + e
                match = ids == expert
                hits.append(jnp.sum(jnp.where(match, 1.0, 0.0), axis=0, keepdims=True))
                picked.append(jnp.sum(jnp.where(match, weights, 0.0), axis=0, keepdims=True))
    hit = jnp.concatenate(hits, axis=0)
    rank = jnp.dot(hit.astype(lower.dtype), lower[...], preferred_element_type=jnp.float32)
    slots = jnp.where(hit > 0.0, rank, -1.0)
    level = lax.broadcasted_iota(jnp.int32, (capacity, block), 0).astype(jnp.float32)
    each = groups * exp_dev
    for c in range(len(chips)):
        for j in range(each):
            i = c * each + j
            flat[c, j * capacity:(j + 1) * capacity, :] = jnp.where(level == slots[i:i + 1, :], picked[i], 0.0)
        table[c] = jnp.transpose(flat[c])

    def place(p, q):
        out = (q % 2) << orders[p][0]
        return out + sum(((q >> (count - k)) & 1) << orders[p][k] for k in range(1, count))

    def multiply(p, low, high):
        c = 1 + firsts.index(orders[p][0])
        spots = [pl.ds(place(p, q) * tok, tok) for q in range(low, high)]
        left = jnp.concatenate(
            [jnp.concatenate([table[x, spot, :] for spot in spots], axis=0) for x in (0, c)], axis=1
        )
        acc[p][low * tok:high * tok, :] = jnp.dot(
            left,
            rows[p][...].reshape(2 * depth, wide[p]),
            preferred_element_type=jnp.float32,
            precision=lax.Precision.HIGHEST,
        )

    def fold(p, k, h):
        size = (n >> k) * tok
        mid = size // 2
        where = pl.ds(size + mid if h == 0 else size, mid)
        return pltpu.make_async_remote_copy(
            src_ref=acc[p].at[where],
            dst_ref=got[p].at[where],
            send_sem=fold_send.at[p, k - 1, h],
            recv_sem=fold_recv.at[p, k - 1, h],
            device_id={"ep": peers[1 << orders[p][k]]},
            device_id_type=MESH,
        )

    def deliver(p, q):
        to = ((q // 2) << orders[p][count - 1]) + ((q % 2) << orders[p][0])
        where = pl.ds(q * tok, tok)
        return pltpu.make_async_remote_copy(
            src_ref=acc[p].at[where],
            dst_ref=got[p].at[where] if q > 1 else last[p],
            send_sem=last_send.at[p, q - 1],
            recv_sem=last_recv.at[p, q - 1],
            device_id={"ep": peers[to]},
            device_id_type=MESH,
        )

    folds = {(p, k, h): fold(p, k, h) for p in range(parts) for k in range(1, count - 1) for h in range(2)}
    lasts = {(p, q): deliver(p, q) for p in range(parts) for q in range(1, 4)}

    def add(p, size, low, high):
        acc[p][low:high, :] += got[p][size + low:size + high, :]

    for p, k, h in FUSED_SEQUENCE:
        size = (n >> k) * tok
        mid = size // 2
        if k == 0:
            loads[p].wait()
            for copy in swaps[p]:
                copy.wait_recv()
            multiply(p, n // 2, n)
            folds[p, 1, 0].start()
            folds[p, 1, 1].start()
            multiply(p, 0, n // 2)
        elif k < count - 2:
            folds[p, k, h].wait_recv()
            if h == 0:
                for half in range(2):
                    low = mid + mid // 2 if half == 0 else mid
                    add(p, size, low, low + mid // 2)
                    folds[p, k + 1, half].start()
            else:
                add(p, size, 0, mid)
        elif k == count - 2:
            folds[p, k, h].wait_recv()
            if h == 0:
                add(p, size, mid, size)
                lasts[p, 3].start()
                lasts[p, 2].start()
            else:
                add(p, size, 0, mid)
                lasts[p, 1].start()
    for p, k, h in FUSED_SEQUENCE:
        if k == count - 1 and h == 0:
            lasts[p, 2].wait_recv()
            o_ref[:, mine(p)] = acc[p][0:tok, :] + got[p][2 * tok:3 * tok, :] + ident * own[:, mine(p)]
        elif k == count:
            lasts[p, 1].wait_recv()
            lasts[p, 3].wait_recv()
            o_ref[:, theirs(p)] = last[p][...] + got[p][3 * tok:4 * tok, :] + ident * own[:, theirs(p)]
    for copy in spread:
        copy.wait_send()
    for p in range(parts):
        for copy in swaps[p]:
            copy.wait_send()
    for copy in list(folds.values()) + list(lasts.values()):
        copy.wait_send()


def fused_fits(n, tok, top, exp_dev, capacity, width, groups):
    half = width // groups
    depth = groups * exp_dev * capacity
    block = n * tok
    firsts = len({order[0] for order in FUSED_ORDERS})
    floats = block * half + depth * half + 2 * (1 + firsts) * depth * block + block * block // 2 + 3 * tok * half
    shapes = 2 * top % 8 == 0 and half % (2 * sum(WIDTHS) * 128) == 0 and depth % 128 == 0 and block % 128 == 0 and tok % 8 == 0
    return n == 1 << FUSED_COUNT and shapes and floats * 4 <= (40 << 20)


def fused(tokens, route_ids, route_weights, expert_rows, count, groups, experts):
    n = 1 << count
    tok, top = route_ids.shape
    exp_dev, capacity, width = expert_rows.shape
    half = width // groups
    wide = [half // (2 * sum(WIDTHS)) * w for w in WIDTHS]
    shapes = ((2 * groups, exp_dev, capacity), (n * tok,), (n * tok,), (tok,))
    depth = groups * exp_dev * capacity
    firsts = sorted({order[0] for order in FUSED_ORDERS})
    chips = 1 + len(firsts)
    anywhere = pl.BlockSpec(memory_space=pl.ANY)
    return pl.pallas_call(
        functools.partial(fused_kernel, count, groups, experts, firsts),
        out_shape=jax.ShapeDtypeStruct((tok, half), jnp.float32),
        in_specs=[anywhere] * 4,
        out_specs=pl.BlockSpec(memory_space=pltpu.VMEM),
        scratch_shapes=[
            pltpu.VMEM((top, tok), jnp.int32),
            pltpu.VMEM((top, tok), jnp.float32),
            pltpu.VMEM((n,) + packed_shape(top, tok), jnp.float32),
            pltpu.VMEM((tok, half), jnp.float32),
            pltpu.VMEM((n * tok, n * tok), jnp.bfloat16),
            pltpu.VMEM((chips, depth, n * tok), jnp.float32),
            pltpu.VMEM((chips, n * tok, depth), jnp.float32),
            pltpu.SemaphoreType.DMA((3,)),
            pltpu.SemaphoreType.DMA((PARTS,)),
            pltpu.SemaphoreType.REGULAR((count - 1,)),
            pltpu.SemaphoreType.DMA((n,)),
            pltpu.SemaphoreType.DMA((n,)),
            pltpu.SemaphoreType.DMA((PARTS, 2 * groups, exp_dev)),
            pltpu.SemaphoreType.DMA((PARTS, 2 * groups, exp_dev)),
            pltpu.SemaphoreType.DMA((PARTS, count - 2, 2)),
            pltpu.SemaphoreType.DMA((PARTS, count - 2, 2)),
            pltpu.SemaphoreType.DMA((PARTS, 3)),
            pltpu.SemaphoreType.DMA((PARTS, 3)),
        ] + [pltpu.VMEM(shape + (w,), jnp.float32) for shape in shapes for w in wide],
        compiler_params=pltpu.CompilerParams(
            collective_id=2, has_side_effects=True, vmem_limit_bytes=53 << 20
        ),
    )(tokens, route_ids.T, route_weights.T, expert_rows)


def shards(tokens, route_ids, route_weights, expert_rows):
    groups = lax.axis_size("grp")
    n = lax.axis_size("ep")
    count = n.bit_length() - 1
    group_index = lax.axis_index("grp")
    ep_index = lax.axis_index("ep")
    exp_dev, capacity, width = expert_rows.shape
    tok, top = route_ids.shape
    experts = exp_dev * groups * n
    half = width // groups
    depth = exp_dev * groups * capacity
    if fused_fits(n, tok, top, exp_dev, capacity, width, groups):
        return fused(tokens, route_ids, route_weights, expert_rows, count, groups, experts)

    packed = jnp.concatenate([route_ids.astype(jnp.float32), route_weights], axis=1)
    lanes = 128 if packed.size % 128 == 0 else packed.shape[1]
    everyone, *swapped = gather_small(packed.reshape(-1, lanes), expert_rows, count, groups)
    everyone = everyone.reshape((n,) + packed.shape)
    owners = [(group_index - d) % groups for d in range(groups)]
    owned = [(g * n + ep_index) * exp_dev + j for g in owners for j in range(exp_dev)]

    ids = everyone[:, :, :top].astype(jnp.int32)
    weights = everyone[:, :, top:]
    homes = jnp.stack([relative(ep_index, r) for r in range(n)])
    earlier_home = (homes[None, :] < homes[:, None]).astype(jnp.float32)
    lower = (jnp.arange(tok)[None, :] < jnp.arange(tok)[:, None]).astype(jnp.float32)
    lane = lax.broadcasted_iota(jnp.int32, (n, tok, depth), 2)
    table = jnp.zeros((n, tok, depth), jnp.float32)
    for j, expert in enumerate(owned):
        match = ids == expert
        hit = jnp.sum(match.astype(jnp.float32), axis=2)
        weight = jnp.sum(jnp.where(match, weights, 0.0), axis=2)
        before = jnp.sum(earlier_home * jnp.sum(hit, axis=1)[None, :], axis=1)
        within = jnp.sum(lower[None, :, :] * hit[:, None, :], axis=2)
        rank = (before[:, None] + within).astype(jnp.int32)
        slot = jnp.where(hit > 0, jnp.minimum(rank, capacity - 1) + j * capacity, -1)
        table = table + jnp.where(lane == slot[:, :, None], weight[:, :, None], 0.0)

    tiles = half // 128
    fits = max(1, (8 << 20) // (n * tok * 128 * 4))
    chunk = max(d for d in range(1, tiles + 1) if tiles % d == 0 and d <= fits)
    parts = max(d for d in range(1, chunk + 1) if chunk % d == 0 and d <= len(ORDERS))
    sums = [
        scatter_sum(table, expert_rows, swapped, count, parts, a * 128, chunk * 128)
        for a in range(0, tiles, chunk)
    ]
    total = sums[0] if len(sums) == 1 else jnp.concatenate(sums, axis=1)
    ident = jnp.sum(jnp.where(route_ids >= experts, route_weights, 0.0), axis=1)
    own_half = lax.dynamic_slice_in_dim(tokens, group_index * half, half, 1)
    return total + ident[:, None] * own_half


def solution(mesh):
    placed = (P("ep", None), P("ep", None), P("ep", None), P(("grp", "ep"), None, None))
    return jax.shard_map(
        shards, mesh=mesh, in_specs=placed, out_specs=P("ep", "grp"), check_vma=False
    )
```

```python
import functools

import jax
import jax.numpy as jnp
from jax import lax
from jax.experimental import pallas as pl
from jax.experimental.pallas import tpu as pltpu
from jax.sharding import PartitionSpec as P

MESH = pl.DeviceIdType.MESH
ORDERS = ((2, 0, 1, 3), (0, 2, 1, 3), (1, 3, 0, 2), (1, 3, 0, 2), (2, 0, 1, 3), (0, 1, 2, 3))


def relative(index, r):
    out, b = index, 0
    while r >> b:
        if (r >> b) & 1:
            out = out + (1 << b) * (1 - 2 * ((index // (1 << b)) % 2))
        b += 1
    return out


def fold_orders(count, parts):
    return [
        [b for b in ORDERS[p % len(ORDERS)] if b < count] + list(range(len(ORDERS[0]), count))
        for p in range(parts)
    ]


def arrival_order(orders, count):
    parts = len(orders)
    ready = [((p + 1) * 0.5, p, 0) for p in range(parts)]
    free = [0.0] * (count + 1)
    events = []
    while ready:
        start, p, s = min(ready)
        ready.remove((start, p, s))
        bit = orders[p][s]
        units = (1 << (count - 1 - s)) * 8.4 / parts
        end = max(start, free[bit]) + (2 * units if bit > 2 else units)
        free[bit] = end
        if bit > 2:
            free[2] = max(start, free[2]) + units
            end = max(end, free[2])
        events.append((end, p, s))
        if s < count - 1:
            ready.append((end + 2.5, p, s + 1))
    return [(p, s) for _, p, s in sorted(events)]


def gather_kernel(count, groups, x_ref, e_ref, o_ref, *rest):
    swapped = rest[:groups - 1]
    send_sem, recv_sem, swap_send, swap_recv = rest[groups - 1:]
    n = 1 << count
    me, grp = lax.axis_index("ep"), lax.axis_index("grp")
    half = e_ref.shape[2] // groups
    peers = [relative(me, r) for r in range(n)]
    barrier = pltpu.get_barrier_semaphore()
    others = [lax.rem(grp + d, groups) for d in range(1, groups)]
    for g in others:
        pl.semaphore_signal(barrier, inc=1, device_id={"grp": g}, device_id_type=MESH)
    for r in range(1, n):
        pl.semaphore_signal(barrier, inc=1, device_id={"ep": peers[r]}, device_id_type=MESH)
    pl.semaphore_wait(barrier, n - 1 + groups - 1)
    copies = []
    for r in range(n - 1, 0, -1):
        copies.append(pltpu.make_async_remote_copy(
            src_ref=x_ref,
            dst_ref=o_ref.at[r],
            send_sem=send_sem.at[r],
            recv_sem=recv_sem.at[r],
            device_id={"ep": peers[r]},
            device_id_type=MESH,
        ))
    for d, g in enumerate(others):
        copies.append(pltpu.make_async_remote_copy(
            src_ref=e_ref.at[:, :, pl.ds(pl.multiple_of(g * half, 128), half)],
            dst_ref=swapped[d],
            send_sem=swap_send.at[d],
            recv_sem=swap_recv.at[d],
            device_id={"grp": g},
            device_id_type=MESH,
        ))
    for copy in copies:
        copy.start()
    o_ref[0] = x_ref[...]
    for copy in copies:
        copy.wait()


def gather_small(x, expert_rows, count, groups):
    n = 1 << count
    exp_dev, capacity, width = expert_rows.shape
    swap = jax.ShapeDtypeStruct((exp_dev, capacity, width // groups), expert_rows.dtype)
    vmem, anywhere = pl.BlockSpec(memory_space=pltpu.VMEM), pl.BlockSpec(memory_space=pl.ANY)
    return pl.pallas_call(
        functools.partial(gather_kernel, count, groups),
        out_shape=[jax.ShapeDtypeStruct((n,) + x.shape, x.dtype)] + [swap] * (groups - 1),
        in_specs=[vmem, anywhere],
        out_specs=[vmem] + [anywhere] * (groups - 1),
        scratch_shapes=[
            pltpu.SemaphoreType.DMA((n,)),
            pltpu.SemaphoreType.DMA((n,)),
            pltpu.SemaphoreType.DMA((groups - 1,)),
            pltpu.SemaphoreType.DMA((groups - 1,)),
        ],
        compiler_params=pltpu.CompilerParams(collective_id=0, has_side_effects=True),
    )(x, expert_rows)


def scatter_kernel(count, parts, groups, column, c_ref, e_ref, *rest):
    swapped = rest[:groups - 1]
    o_ref, rows, acc, got, load_sem, send_sem, recv_sem = rest[groups - 1:]
    n = 1 << count
    tok = c_ref.shape[1]
    exp_dev, capacity, width = e_ref.shape
    half_width = width // groups
    wide = acc.shape[2]
    me, grp = lax.axis_index("ep"), lax.axis_index("grp")

    def loads(p):
        out = []
        start = column + p * wide
        for i in range(groups * exp_dev):
            g, e = i // exp_dev, i % exp_dev
            if g == 0:
                src = e_ref.at[e, :, pl.ds(pl.multiple_of(grp * half_width + start, 128), wide)]
            else:
                src = swapped[g - 1].at[e, :, pl.ds(start, wide)]
            dst = rows.at[p, pl.ds(i * capacity, capacity)]
            out.append(pltpu.make_async_copy(src, dst, load_sem.at[p, i]))
        return out

    loading = [loads(p) for p in range(parts)]
    for p in range(parts):
        for copy in loading[p]:
            copy.start()

    peers = [relative(me, 1 << b) for b in range(count)]
    barrier = pltpu.get_barrier_semaphore()
    for b in range(count):
        pl.semaphore_signal(barrier, inc=1, device_id={"ep": peers[b]}, device_id_type=MESH)
    orders = fold_orders(count, parts)

    def place(p, q):
        return sum(((q >> (count - 1 - s)) & 1) << orders[p][s] for s in range(count))

    def multiply(p, low, high):
        weights = jnp.concatenate([c_ref[place(p, q)] for q in range(low, high)], axis=0)
        acc[p, low * tok:high * tok, :] = jnp.dot(
            weights,
            rows[p],
            preferred_element_type=jnp.float32,
            precision=lax.Precision.HIGHEST,
        )

    def transfer(p, s):
        half = (n >> (s + 1)) * tok
        return pltpu.make_async_remote_copy(
            src_ref=acc.at[p, pl.ds(half, half)],
            dst_ref=got.at[p, pl.ds(half, half)],
            send_sem=send_sem.at[p, s],
            recv_sem=recv_sem.at[p, s],
            device_id={"ep": peers[orders[p][s]]},
            device_id_type=MESH,
        )

    copies = [[transfer(p, s) for s in range(count)] for p in range(parts)]
    for p in range(parts):
        for copy in loading[p]:
            copy.wait()
        multiply(p, n // 2, n)
        if p == 0:
            pl.semaphore_wait(barrier, count)
        copies[p][0].start()
    for p in range(parts):
        multiply(p, 0, n // 2)
    for p, s in arrival_order(orders, count):
        half = (n >> (s + 1)) * tok
        copies[p][s].wait_recv()
        if s < count - 1:
            mid = half // 2
            acc[p, mid:half, :] += got[p, half + mid:2 * half, :]
            copies[p][s + 1].start()
            acc[p, 0:mid, :] += got[p, half:half + mid, :]
        else:
            o_ref[:, p * wide:(p + 1) * wide] = acc[p, 0:tok, :] + got[p, tok:2 * tok, :]
    for p in range(parts):
        for s in range(count):
            copies[p][s].wait_send()


def scatter_sum(c, expert_rows, swapped, count, parts, column, span):
    n, tok, depth = c.shape
    groups = len(swapped) + 1
    wide = span // parts
    vmem, anywhere = pl.BlockSpec(memory_space=pltpu.VMEM), pl.BlockSpec(memory_space=pl.ANY)
    return pl.pallas_call(
        functools.partial(scatter_kernel, count, parts, groups, column),
        out_shape=jax.ShapeDtypeStruct((tok, span), jnp.float32),
        in_specs=[vmem, anywhere] + [anywhere] * (groups - 1),
        out_specs=vmem,
        scratch_shapes=[
            pltpu.VMEM((parts, depth, wide), jnp.float32),
            pltpu.VMEM((parts, n * tok, wide), jnp.float32),
            pltpu.VMEM((parts, n * tok, wide), jnp.float32),
            pltpu.SemaphoreType.DMA((parts, groups * expert_rows.shape[0])),
            pltpu.SemaphoreType.DMA((parts, count)),
            pltpu.SemaphoreType.DMA((parts, count)),
        ],
        compiler_params=pltpu.CompilerParams(
            collective_id=1, has_side_effects=True, vmem_limit_bytes=60 << 20
        ),
    )(c, expert_rows, *swapped)


WIDTHS = (2, 2, 2, 2, 2, 2)
PARTS = len(WIDTHS)
FUSED_COUNT = 4
EARLY = 6
FUSED_ORDERS = (
        (1, 3, 0, 2), (2, 0, 1, 3), (1, 0, 2, 3), (2, 0, 1, 3), (0, 1, 2, 3), (0, 1, 2, 3),
)
FUSED_SEQUENCE = (
        (0, 0, 0), (1, 0, 0), (4, 0, 0), (2, 0, 0), (5, 0, 0), (4, 1, 0), (1, 1, 0), (4, 1, 1), (1, 1, 1), (3, 0, 0),
        (0, 1, 0), (2, 1, 0), (0, 1, 1), (5, 1, 0), (4, 2, 0), (2, 1, 1), (4, 2, 1), (5, 1, 1), (1, 2, 0), (2, 2, 0),
        (1, 2, 1), (3, 1, 0), (2, 2, 1), (0, 2, 0), (5, 2, 0), (3, 1, 1), (3, 2, 0), (0, 2, 1), (3, 2, 1), (5, 2, 1),
        (0, 3, 0), (0, 4, 0), (1, 3, 0), (1, 4, 0), (2, 3, 0), (2, 4, 0), (3, 3, 0), (3, 4, 0), (4, 3, 0), (4, 4, 0),
        (5, 3, 0), (5, 4, 0),
)


def packed_shape(top, tok):
    return (8, -(-(2 * top // 8) * tok // 128) * 128)


def pack(both, shape):
    blocks = [both[i:i + 8] for i in range(0, both.shape[0], 8)]
    room = shape[1] - len(blocks) * both.shape[1]
    if room:
        blocks.append(jnp.zeros((8, room), both.dtype))
    return jnp.concatenate(blocks, axis=1)


def unpack(tile, height, tok):
    return jnp.concatenate([tile[:, i * tok:(i + 1) * tok] for i in range(height // 8)], axis=0)


def fused_kernel(count, groups, experts, firsts, t_ref, i_ref, w_ref, e_ref, o_ref, ids_own, w_own, packed,
                 own, lower, flat, table, small_sem, load_sem, present, gather_send, gather_recv,
                 swap_send, swap_recv, fold_send, fold_recv, last_send, last_recv, *buffers):
    n = 1 << count
    top, tok = i_ref.shape
    exp_dev, capacity, width = e_ref.shape
    half_width = width // groups
    parts = PARTS
    rows, acc, got, last = [buffers[i * parts:(i + 1) * parts] for i in range(4)]
    wide = [ref.shape[1] for ref in acc]
    first = [2 * sum(wide[:p]) for p in range(parts)]
    depth = groups * exp_dev * capacity
    orders = FUSED_ORDERS
    me, grp = lax.axis_index("ep"), lax.axis_index("grp")
    peers = [relative(me, r) for r in range(n)]
    others = [lax.rem(grp + d, groups) for d in range(1, groups)]
    sides = [lax.rem(me // (1 << orders[p][0]), 2) for p in range(parts)]

    def mine(p):
        return pl.ds(pl.multiple_of(first[p] + sides[p] * wide[p], 128), wide[p])

    def theirs(p):
        return pl.ds(pl.multiple_of(first[p] + (1 - sides[p]) * wide[p], 128), wide[p])

    def source(g, p, side):
        return e_ref.at[:, :, pl.ds(pl.multiple_of(g * half_width + first[p] + side * wide[p], 128), wide[p])]

    smalls = [
        pltpu.make_async_copy(i_ref, ids_own, small_sem.at[0]),
        pltpu.make_async_copy(w_ref, w_own, small_sem.at[1]),
        pltpu.make_async_copy(
            t_ref.at[:, pl.ds(pl.multiple_of(grp * half_width, 128), half_width)], own, small_sem.at[2]
        ),
    ]
    for copy in smalls:
        copy.start()
    barrier = pltpu.get_barrier_semaphore()
    for b in range(count):
        pl.semaphore_signal(barrier, inc=1, device_id={"ep": peers[1 << b]}, device_id_type=MESH)
    for g in others:
        for b in firsts:
            pl.semaphore_signal(barrier, inc=1, device_id={"grp": g, "ep": peers[1 << b]}, device_id_type=MESH)
        pl.semaphore_signal(barrier, inc=1, device_id={"grp": g}, device_id_type=MESH)

    loads = [pltpu.make_async_copy(source(grp, p, sides[p]), rows[p].at[0], load_sem.at[p]) for p in range(parts)]
    for copy in loads:
        copy.start()

    block = n * tok
    across = jnp.concatenate(
        [lax.broadcasted_iota(jnp.int32, (1, tok), 1) + peers[r] * tok for r in range(n)], axis=1
    )
    down = jnp.concatenate(
        [lax.broadcasted_iota(jnp.int32, (tok, 1), 0) + peers[r] * tok for r in range(n)], axis=0
    )
    lower[...] = jnp.where(down < across, 1.0, 0.0).astype(lower.dtype)

    smalls[0].wait()
    smalls[1].wait()
    both = jnp.concatenate([ids_own[...].astype(jnp.float32), w_own[...]], axis=0)
    packed[0] = pack(both, packed.shape[1:])
    pl.semaphore_wait(barrier, count + (groups - 1) * (1 + len(firsts)))
    def swap(p, slot, e):
        c, d = slot // groups, slot % groups
        to = {}
        if c:
            to["ep"] = peers[1 << orders[p][0]]
        if d:
            to["grp"] = others[d - 1]
        return pltpu.make_async_remote_copy(
            src_ref=source(lax.rem(grp + d, groups), p, 1 - sides[p] if c else sides[p]).at[e],
            dst_ref=rows[p].at[slot, e],
            send_sem=swap_send.at[p, slot, e],
            recv_sem=swap_recv.at[p, slot, e],
            device_id=to,
            device_id_type=MESH,
        )

    swaps = [
        [swap(p, slot, e) for slot in range(2 * groups - 1, 0, -1) for e in range(exp_dev)] for p in range(parts)
    ]
    far = groups * exp_dev
    queues = [[(p, i) for p in range(parts) if orders[p][0] == b for i in range(far)] for b in firsts]
    early = [
        (p, i) for queue in queues for at, (p, i) in enumerate(queue)
        if sum(wide[x] for x, _ in queue[:at]) < half_width // EARLY
    ]
    later = [(p, i) for p in range(parts) for i in range(len(swaps[p])) if (p, i) not in early]
    for p, i in early:
        swaps[p][i].start()
    for p in range(parts):
        for i in range(far, len(swaps[p])):
            swaps[p][i].start()
    for b in range(count - 2, -1, -1):
        pl.semaphore_signal(present.at[b], inc=1, device_id={"ep": peers[1 << b]}, device_id_type=MESH)
        pl.semaphore_wait(present.at[b], 1)
    spread = []
    for r in range(n - 1, 0, -1):
        spread.append(pltpu.make_async_remote_copy(
            src_ref=packed.at[0],
            dst_ref=packed.at[r],
            send_sem=gather_send.at[r],
            recv_sem=gather_recv.at[r],
            device_id={"ep": peers[r]},
            device_id_type=MESH,
        ))
        spread[-1].start()
    for p, i in later:
        if i < far:
            swaps[p][i].start()

    chosen = ids_own[...]
    ident_row = jnp.sum(jnp.where(chosen >= experts, w_own[...], 0.0), axis=0, keepdims=True)
    eye = lax.broadcasted_iota(jnp.int32, (tok, tok), 0) == lax.broadcasted_iota(jnp.int32, (tok, tok), 1)
    ident = jnp.sum(jnp.where(eye, ident_row, 0.0), axis=1, keepdims=True)
    smalls[2].wait()

    for copy in spread:
        copy.wait_recv()
    both = jnp.concatenate([both] + [unpack(packed[r], 2 * top, tok) for r in range(1, n)], axis=1)
    ids = both[:top].astype(jnp.int32)
    weights = both[top:]
    chips = [me] + [peers[1 << b] for b in firsts]
    hits, picked = [], []
    for chip in chips:
        for d in range(groups):
            for e in range(exp_dev):
                expert = (lax.rem(grp + groups - d, groups) * n + chip) * exp_dev + e
                match = ids == expert
                hits.append(jnp.sum(jnp.where(match, 1.0, 0.0), axis=0, keepdims=True))
                picked.append(jnp.sum(jnp.where(match, weights, 0.0), axis=0, keepdims=True))
    hit = jnp.concatenate(hits, axis=0)
    rank = jnp.dot(hit.astype(lower.dtype), lower[...], preferred_element_type=jnp.float32)
    slots = jnp.where(hit > 0.0, rank, -1.0)
    level = lax.broadcasted_iota(jnp.int32, (capacity, block), 0).astype(jnp.float32)
    each = groups * exp_dev
    for c in range(len(chips)):
        for j in range(each):
            i = c * each + j
            flat[c, j * capacity:(j + 1) * capacity, :] = jnp.where(level == slots[i:i + 1, :], picked[i], 0.0)
        table[c] = jnp.transpose(flat[c])

    def place(p, q):
        out = (q % 2) << orders[p][0]
        return out + sum(((q >> (count - k)) & 1) << orders[p][k] for k in range(1, count))

    def multiply(p, low, high):
        c = 1 + firsts.index(orders[p][0])
        spots = [pl.ds(place(p, q) * tok, tok) for q in range(low, high)]
        left = jnp.concatenate(
            [jnp.concatenate([table[x, spot, :] for spot in spots], axis=0) for x in (0, c)], axis=1
        )
        acc[p][low * tok:high * tok, :] = jnp.dot(
            left,
            rows[p][...].reshape(2 * depth, wide[p]),
            preferred_element_type=jnp.float32,
            precision=lax.Precision.HIGHEST,
        )

    def fold(p, k, h):
        size = (n >> k) * tok
        mid = size // 2
        where = pl.ds(size + mid if h == 0 else size, mid)
        return pltpu.make_async_remote_copy(
            src_ref=acc[p].at[where],
            dst_ref=got[p].at[where],
            send_sem=fold_send.at[p, k - 1, h],
            recv_sem=fold_recv.at[p, k - 1, h],
            device_id={"ep": peers[1 << orders[p][k]]},
            device_id_type=MESH,
        )

    def deliver(p, q):
        to = ((q // 2) << orders[p][count - 1]) + ((q % 2) << orders[p][0])
        where = pl.ds(q * tok, tok)
        return pltpu.make_async_remote_copy(
            src_ref=acc[p].at[where],
            dst_ref=got[p].at[where] if q > 1 else last[p],
            send_sem=last_send.at[p, q - 1],
            recv_sem=last_recv.at[p, q - 1],
            device_id={"ep": peers[to]},
            device_id_type=MESH,
        )

    folds = {(p, k, h): fold(p, k, h) for p in range(parts) for k in range(1, count - 1) for h in range(2)}
    lasts = {(p, q): deliver(p, q) for p in range(parts) for q in range(1, 4)}

    def add(p, size, low, high):
        acc[p][low:high, :] += got[p][size + low:size + high, :]

    for p, k, h in FUSED_SEQUENCE:
        size = (n >> k) * tok
        mid = size // 2
        if k == 0:
            loads[p].wait()
            for copy in swaps[p]:
                copy.wait_recv()
            multiply(p, n // 2, n)
            folds[p, 1, 0].start()
            folds[p, 1, 1].start()
            multiply(p, 0, n // 2)
        elif k < count - 2:
            folds[p, k, h].wait_recv()
            if h == 0:
                for half in range(2):
                    low = mid + mid // 2 if half == 0 else mid
                    add(p, size, low, low + mid // 2)
                    folds[p, k + 1, half].start()
            else:
                add(p, size, 0, mid)
        elif k == count - 2:
            folds[p, k, h].wait_recv()
            if h == 0:
                add(p, size, mid, size)
                lasts[p, 3].start()
                lasts[p, 2].start()
            else:
                add(p, size, 0, mid)
                lasts[p, 1].start()
    for p, k, h in FUSED_SEQUENCE:
        if k == count - 1 and h == 0:
            lasts[p, 2].wait_recv()
            o_ref[:, mine(p)] = acc[p][0:tok, :] + got[p][2 * tok:3 * tok, :] + ident * own[:, mine(p)]
        elif k == count:
            lasts[p, 1].wait_recv()
            lasts[p, 3].wait_recv()
            o_ref[:, theirs(p)] = last[p][...] + got[p][3 * tok:4 * tok, :] + ident * own[:, theirs(p)]
    for copy in spread:
        copy.wait_send()
    for p in range(parts):
        for copy in swaps[p]:
            copy.wait_send()
    for copy in list(folds.values()) + list(lasts.values()):
        copy.wait_send()


def fused_fits(n, tok, top, exp_dev, capacity, width, groups):
    half = width // groups
    depth = groups * exp_dev * capacity
    block = n * tok
    firsts = len({order[0] for order in FUSED_ORDERS})
    floats = block * half + depth * half + 2 * (1 + firsts) * depth * block + block * block // 2 + 3 * tok * half
    shapes = 2 * top % 8 == 0 and half % (2 * sum(WIDTHS) * 128) == 0 and depth % 128 == 0 and block % 128 == 0 and tok % 8 == 0
    return n == 1 << FUSED_COUNT and shapes and floats * 4 <= (40 << 20)


def fused(tokens, route_ids, route_weights, expert_rows, count, groups, experts):
    n = 1 << count
    tok, top = route_ids.shape
    exp_dev, capacity, width = expert_rows.shape
    half = width // groups
    wide = [half // (2 * sum(WIDTHS)) * w for w in WIDTHS]
    shapes = ((2 * groups, exp_dev, capacity), (n * tok,), (n * tok,), (tok,))
    depth = groups * exp_dev * capacity
    firsts = sorted({order[0] for order in FUSED_ORDERS})
    chips = 1 + len(firsts)
    anywhere = pl.BlockSpec(memory_space=pl.ANY)
    return pl.pallas_call(
        functools.partial(fused_kernel, count, groups, experts, firsts),
        out_shape=jax.ShapeDtypeStruct((tok, half), jnp.float32),
        in_specs=[anywhere] * 4,
        out_specs=pl.BlockSpec(memory_space=pltpu.VMEM),
        scratch_shapes=[
            pltpu.VMEM((top, tok), jnp.int32),
            pltpu.VMEM((top, tok), jnp.float32),
            pltpu.VMEM((n,) + packed_shape(top, tok), jnp.float32),
            pltpu.VMEM((tok, half), jnp.float32),
            pltpu.VMEM((n * tok, n * tok), jnp.bfloat16),
            pltpu.VMEM((chips, depth, n * tok), jnp.float32),
            pltpu.VMEM((chips, n * tok, depth), jnp.float32),
            pltpu.SemaphoreType.DMA((3,)),
            pltpu.SemaphoreType.DMA((PARTS,)),
            pltpu.SemaphoreType.REGULAR((count - 1,)),
            pltpu.SemaphoreType.DMA((n,)),
            pltpu.SemaphoreType.DMA((n,)),
            pltpu.SemaphoreType.DMA((PARTS, 2 * groups, exp_dev)),
            pltpu.SemaphoreType.DMA((PARTS, 2 * groups, exp_dev)),
            pltpu.SemaphoreType.DMA((PARTS, count - 2, 2)),
            pltpu.SemaphoreType.DMA((PARTS, count - 2, 2)),
            pltpu.SemaphoreType.DMA((PARTS, 3)),
            pltpu.SemaphoreType.DMA((PARTS, 3)),
        ] + [pltpu.VMEM(shape + (w,), jnp.float32) for shape in shapes for w in wide],
        compiler_params=pltpu.CompilerParams(
            collective_id=2, has_side_effects=True, vmem_limit_bytes=53 << 20
        ),
    )(tokens, route_ids.T, route_weights.T, expert_rows)


def shards(tokens, route_ids, route_weights, expert_rows):
    groups = lax.axis_size("grp")
    n = lax.axis_size("ep")
    count = n.bit_length() - 1
    group_index = lax.axis_index("grp")
    ep_index = lax.axis_index("ep")
    exp_dev, capacity, width = expert_rows.shape
    tok, top = route_ids.shape
    experts = exp_dev * groups * n
    half = width // groups
    depth = exp_dev * groups * capacity
    if fused_fits(n, tok, top, exp_dev, capacity, width, groups):
        return fused(tokens, route_ids, route_weights, expert_rows, count, groups, experts)

    packed = jnp.concatenate([route_ids.astype(jnp.float32), route_weights], axis=1)
    lanes = 128 if packed.size % 128 == 0 else packed.shape[1]
    everyone, *swapped = gather_small(packed.reshape(-1, lanes), expert_rows, count, groups)
    everyone = everyone.reshape((n,) + packed.shape)
    owners = [(group_index - d) % groups for d in range(groups)]
    owned = [(g * n + ep_index) * exp_dev + j for g in owners for j in range(exp_dev)]

    ids = everyone[:, :, :top].astype(jnp.int32)
    weights = everyone[:, :, top:]
    homes = jnp.stack([relative(ep_index, r) for r in range(n)])
    earlier_home = (homes[None, :] < homes[:, None]).astype(jnp.float32)
    lower = (jnp.arange(tok)[None, :] < jnp.arange(tok)[:, None]).astype(jnp.float32)
    lane = lax.broadcasted_iota(jnp.int32, (n, tok, depth), 2)
    table = jnp.zeros((n, tok, depth), jnp.float32)
    for j, expert in enumerate(owned):
        match = ids == expert
        hit = jnp.sum(match.astype(jnp.float32), axis=2)
        weight = jnp.sum(jnp.where(match, weights, 0.0), axis=2)
        before = jnp.sum(earlier_home * jnp.sum(hit, axis=1)[None, :], axis=1)
        within = jnp.sum(lower[None, :, :] * hit[:, None, :], axis=2)
        rank = (before[:, None] + within).astype(jnp.int32)
        slot = jnp.where(hit > 0, jnp.minimum(rank, capacity - 1) + j * capacity, -1)
        table = table + jnp.where(lane == slot[:, :, None], weight[:, :, None], 0.0)

    tiles = half // 128
    fits = max(1, (8 << 20) // (n * tok * 128 * 4))
    chunk = max(d for d in range(1, tiles + 1) if tiles % d == 0 and d <= fits)
    parts = max(d for d in range(1, chunk + 1) if chunk % d == 0 and d <= len(ORDERS))
    sums = [
        scatter_sum(table, expert_rows, swapped, count, parts, a * 128, chunk * 128)
        for a in range(0, tiles, chunk)
    ]
    total = sums[0] if len(sums) == 1 else jnp.concatenate(sums, axis=1)
    ident = jnp.sum(jnp.where(route_ids >= experts, route_weights, 0.0), axis=1)
    own_half = lax.dynamic_slice_in_dim(tokens, group_index * half, half, 1)
    return total + ident[:, None] * own_half


def solution(mesh):
    placed = (P("ep", None), P("ep", None), P("ep", None), P(("grp", "ep"), None, None))
    return jax.shard_map(
        shards, mesh=mesh, in_specs=placed, out_specs=P("ep", "grp"), check_vma=False
    )
```
